32 devices in a mesh: dp: 2 (over x), tp: 4 (over z), cp: 4 (over y, core).
Axes of the slice: x: 2, y: 2, z: 4, core: 2. Of those that a mesh axis runs over, the one named last changes fastest.
Arguments:
- hidden: bfloat16 [24, 24, 8192], P('dp'), parts along dimension 0
- attn_gain: bfloat16 [8192], replicated
- w_query: bfloat16 [8192, 8192], P(None, 'tp')
- w_key: bfloat16 [8192, 1024], P(None, 'tp')
- w_value: bfloat16 [8192, 1024], P(None, 'tp')
- w_out: bfloat16 [8192, 8192], P('tp')
- cache_k: bfloat16 [24, 4, 4, 8, 256, 128], P('dp', None, 'cp', 'tp'), parts along dimension 0
- cache_v: bfloat16 [24, 4, 4, 8, 256, 128], P('dp', None, 'cp', 'tp'), parts along dimension 0
- ctx_len: int32 [24], P('dp'), parts along dimension 0
- positions: int32 [24, 24], P('dp'), parts along dimension 0
- tree_mask: int32 [24, 24, 24], P('dp'), parts along dimension 0
Outputs:
- output 1: bfloat16 [24, 24, 8192], P('dp'), parts along dimension 0
- output 2: bfloat16 [24, 4, 4, 8, 256, 128], P('dp', None, 'cp', 'tp'), parts along dimension 0
- output 3: bfloat16 [24, 4, 4, 8, 256, 128], P('dp', None, 'cp', 'tp'), parts along dimension 0
There are 2 independent parts. The reference program is written for one: setup_inputs(seed, part) draws one part's arguments, and reference() takes and returns one part's arrays. A program takes and returns all parts, laid end to end along the dimension named above; an argument that names none is the same for every part.
All inputs are finite; a program needn't handle non-finite values.
Results may differ from the reference program's by a relative error of at most 0.00843603.
Values sent between devices are 32-bit elements.
A program may use at most 1 GiB of HBM per device.

```python
import math
import jax
import jax.numpy as jnp
from jax import lax

D = 8192
HEADS = 64
KV_HEADS = 8
HEAD = 128
REQ = 12
TREE = 24
BLOCKS_DEV = 4
CP = 4
TP = 4
BLOCK = 256
ROPE_THETA = 500000.0
NORM_EPS = 1e-5
MASKED = -1e30


def rope_tables(positions, head_dim):
    freq_idx = jnp.arange(head_dim // 2, dtype=jnp.float32)
    inv_freq = 1.0 / (ROPE_THETA ** (2.0 * freq_idx / head_dim))
    wavelen = 2.0 * math.pi / inv_freq
    smooth = (8192.0 / wavelen - 1.0) / 3.0
    blended = (1.0 - smooth) * inv_freq / 8.0 + smooth * inv_freq
    inv_freq = jnp.where(wavelen < 2048.0, inv_freq, jnp.where(wavelen > 8192.0, inv_freq / 8.0, blended))
    angle = positions.astype(jnp.float32)[..., None] * inv_freq
    return jnp.cos(angle)[..., None, :], jnp.sin(angle)[..., None, :]


def apply_rope(values, cos_tab, sin_tab):
    half = values.shape[-1] // 2
    first = values[..., :half]
    second = values[..., half:]
    return jnp.concatenate([first * cos_tab - second * sin_tab, second * cos_tab + first * sin_tab], axis=-1)


def rms_norm(hidden, attn_gain):
    wide = hidden.astype(jnp.float32)
    inv_rms = lax.rsqrt(jnp.mean(wide * wide, axis=-1, keepdims=True) + NORM_EPS)
    return wide, (wide * inv_rms * attn_gain.astype(jnp.float32)).astype(jnp.bfloat16)


def draw_structure(key):
    ctx_key, tree_key = jax.random.split(key)
    max_len = BLOCKS_DEV * CP * BLOCK
    ctx_len = jax.random.randint(ctx_key, (REQ,), max_len // 2, max_len - TREE + 1, dtype=jnp.int32)
    ctx_len = ctx_len.at[0].set(max_len - TREE).at[1].set(max_len // 2)
    raw = jax.random.randint(tree_key, (REQ, TREE), 0, 1 << 30, dtype=jnp.int32)
    node_ids = jnp.arange(TREE, dtype=jnp.int32)
    parents = raw % jnp.maximum(node_ids, 1)[None, :]
    ancestry = jnp.broadcast_to(jnp.eye(TREE, dtype=jnp.int32), (REQ, TREE, TREE))
    for node in range(1, TREE):
        above = jnp.take_along_axis(ancestry, parents[:, node][:, None, None], axis=1)[:, 0, :]
        ancestry = ancestry.at[:, node, :].add(above)
    depth = ancestry.sum(axis=-1) - 1
    positions = ctx_len[:, None] + depth
    return ctx_len, positions.astype(jnp.int32), ancestry


def setup_inputs(seed: int = 0, part: int = 0) -> dict:
    base = jax.random.key(seed)
    part_key = jax.random.fold_in(base, part)
    wkeys = jax.random.split(base, 5)
    pkeys = jax.random.split(part_key, 4)
    max_len = BLOCKS_DEV * CP * BLOCK
    key_scale = math.sqrt(math.log(max_len / 64.0))
    new_scale = math.log(max_len) - 1.4
    ctx_len, positions, tree_mask = draw_structure(pkeys[0])
    hidden = (0.5 * jax.random.normal(pkeys[1], (REQ, TREE, D), jnp.float32)).astype(jnp.bfloat16)
    attn_gain = (1.0 + 0.3 * jax.random.normal(wkeys[0], (D,), jnp.float32)).astype(jnp.bfloat16)
    w_query = (jax.random.normal(wkeys[1], (D, HEADS * HEAD), jnp.float32) * D ** -0.5).astype(jnp.bfloat16)
    w_key = (jax.random.normal(wkeys[2], (D, KV_HEADS * HEAD), jnp.float32) * (new_scale * D ** -0.5)).astype(jnp.bfloat16)
    w_value = (jax.random.normal(wkeys[3], (D, KV_HEADS * HEAD), jnp.float32) * (2.0 * D ** -0.5)).astype(jnp.bfloat16)
    w_out = (jax.random.normal(wkeys[4], (HEADS * HEAD, D), jnp.float32) * (HEADS * HEAD) ** -0.5).astype(jnp.bfloat16)
    cache_shape = (REQ, BLOCKS_DEV, CP, KV_HEADS, BLOCK, HEAD)
    cache_k = (key_scale * jax.random.normal(pkeys[2], cache_shape, jnp.float32)).astype(jnp.bfloat16)
    cache_v = (4.0 * jax.random.normal(pkeys[3], cache_shape, jnp.float32)).astype(jnp.bfloat16)
    return {'hidden': hidden, 'attn_gain': attn_gain, 'w_query': w_query, 'w_key': w_key, 'w_value': w_value, 'w_out': w_out, 'cache_k': cache_k, 'cache_v': cache_v, 'ctx_len': ctx_len, 'positions': positions, 'tree_mask': tree_mask}


def reference(hidden, attn_gain, w_query, w_key, w_value, w_out, cache_k, cache_v, ctx_len, positions, tree_mask):
    group = HEADS // KV_HEADS
    max_len = BLOCKS_DEV * CP * BLOCK
    scale = HEAD ** -0.5
    wide, normed = rms_norm(hidden, attn_gain)
    flat_rows = normed.reshape(REQ * TREE, D)
    query = jnp.dot(flat_rows, w_query, preferred_element_type=jnp.float32).reshape(REQ, TREE, HEADS, HEAD)
    key_new = jnp.dot(flat_rows, w_key, preferred_element_type=jnp.float32).reshape(REQ, TREE, KV_HEADS, HEAD)
    val_new = jnp.dot(flat_rows, w_value, preferred_element_type=jnp.float32).astype(jnp.bfloat16).reshape(REQ, TREE, KV_HEADS, HEAD)
    cos_tab, sin_tab = rope_tables(positions, HEAD)
    query = apply_rope(query, cos_tab, sin_tab).astype(jnp.bfloat16)
    key_new = apply_rope(key_new, cos_tab, sin_tab).astype(jnp.bfloat16)

    def attend_one(item):
        q_one, key_one, val_one, cache_k_one, cache_v_one, ctx_one, mask_one = item
        keys_all = jnp.transpose(cache_k_one, (0, 1, 3, 2, 4)).reshape(max_len, KV_HEADS, HEAD).astype(jnp.float32)
        vals_all = jnp.transpose(cache_v_one, (0, 1, 3, 2, 4)).reshape(max_len, KV_HEADS, HEAD).astype(jnp.float32)
        q_wide = q_one.reshape(TREE, KV_HEADS, group, HEAD).astype(jnp.float32)
        score_cache = jnp.einsum('tkgd,lkd->tkgl', q_wide, keys_all) * scale
        valid = jnp.arange(max_len) < ctx_one
        score_cache = jnp.where(valid, score_cache, MASKED)
        score_tree = jnp.einsum('tkgd,skd->tkgs', q_wide, key_one.astype(jnp.float32)) * scale
        tree_ok = (mask_one > 0)[:, None, None, :]
        score_tree = jnp.where(tree_ok, score_tree, MASKED)
        row_max = jnp.maximum(score_cache.max(axis=-1), score_tree.max(axis=-1))
        prob_cache = jnp.exp(score_cache - row_max[..., None])
        prob_tree = jnp.exp(score_tree - row_max[..., None])
        row_sum = prob_cache.sum(axis=-1) + prob_tree.sum(axis=-1)
        mixed = jnp.einsum('tkgl,lkd->tkgd', prob_cache, vals_all) + jnp.einsum('tkgs,skd->tkgd', prob_tree, val_one.astype(jnp.float32))
        return (mixed / row_sum[..., None]).reshape(TREE, HEADS * HEAD).astype(jnp.bfloat16)

    attn = lax.map(attend_one, (query, key_new, val_new, cache_k, cache_v, ctx_len, tree_mask))
    head_part = HEADS * HEAD // TP
    grouped = attn.reshape(REQ, TREE, TP, head_part).astype(jnp.float32)
    proj = jnp.einsum('rtgf,gfe->rtge', grouped, w_out.reshape(TP, head_part, D).astype(jnp.float32)).astype(jnp.bfloat16)
    out_hidden = (wide + proj.astype(jnp.float32).sum(axis=2)).astype(jnp.bfloat16)
    slot_ids = ctx_len[:, None] + jnp.arange(TREE)[None, :]
    block_ids = slot_ids // BLOCK
    req_ids = jnp.broadcast_to(jnp.arange(REQ)[:, None], (REQ, TREE))
    new_cache_k = cache_k.at[req_ids, block_ids // CP, block_ids % CP, :, slot_ids % BLOCK, :].set(key_new)
    new_cache_v = cache_v.at[req_ids, block_ids // CP, block_ids % CP, :, slot_ids % BLOCK, :].set(val_new)
    return (out_hidden, new_cache_k, new_cache_v)
```

```python
import math
import jax
import jax.numpy as jnp
from jax import lax
from jax.experimental import pallas as pl
from jax.experimental.pallas import tpu as pltpu
from jax.sharding import PartitionSpec as P

ROPE_THETA = 500000.0
NORM_EPS = 1e-5
MASKED = -1e30
LOG2E = 1.4426950408889634
MESH = pl.DeviceIdType.MESH

REQ = 12
TREE = 24
ROWS = REQ * TREE
D = 8192
HEAD = 128
KV = 2
GROUP = 8
HEADS = KV * GROUP
NBLK = 4
BLK = 256
CP = 4
WIDE = HEADS * HEAD
EXT = WIDE + HEAD
TILE = 256
NTILE = (HEADS + 2 * KV) * HEAD // TILE
RING = 4
HALF = D // 2
MINE = ROWS // 2
NP = 16
W = HALF // NP


def rope_tables(positions):
    freq_idx = jnp.arange(HEAD // 2, dtype=jnp.float32)
    inv_freq = 1.0 / (ROPE_THETA ** (2.0 * freq_idx / HEAD))
    wavelen = 2.0 * math.pi / inv_freq
    smooth = (8192.0 / wavelen - 1.0) / 3.0
    blended = (1.0 - smooth) * inv_freq / 8.0 + smooth * inv_freq
    inv_freq = jnp.where(wavelen < 2048.0, inv_freq, jnp.where(wavelen > 8192.0, inv_freq / 8.0, blended))
    angle = positions.astype(jnp.float32).reshape(ROWS, 1) * inv_freq
    cos_tab, sin_tab = jnp.cos(angle), jnp.sin(angle)
    return jnp.concatenate([cos_tab, cos_tab], axis=-1), jnp.concatenate([-sin_tab, sin_tab], axis=-1)


def attend_kernel(ctx_ref, gain_ref, cos_ref, sin_ref, mask_ref, x_hbm, wq_hbm, wk_hbm, wv_hbm, ck_hbm, cv_hbm,
                  o_hbm, nk_hbm, nv_hbm,
                  x_ref, h_ref, wbuf, qkv, kbuf, vbuf, obuf, xsem, wsem, ksem, vsem, nksem, nvsem, osem):
    cp_rank = lax.axis_index('cp')
    nq = HEADS * HEAD // TILE

    x_copy = pltpu.make_async_copy(x_hbm, x_ref, xsem)
    x_copy.start()

    def start_weight(i):
        slot = lax.rem(i, RING)

        @pl.when(i < nq)
        def _():
            cols = pl.ds(pl.multiple_of(i * TILE, TILE), TILE)
            pltpu.make_async_copy(wq_hbm.at[:, cols], wbuf.at[slot], wsem.at[slot]).start()

        @pl.when(i == nq)
        def _():
            pltpu.make_async_copy(wk_hbm, wbuf.at[slot], wsem.at[slot]).start()

        @pl.when(i == nq + 1)
        def _():
            pltpu.make_async_copy(wv_hbm, wbuf.at[slot], wsem.at[slot]).start()

    def start_cache(r):
        pltpu.make_async_copy(ck_hbm.at[r, :, 0], kbuf.at[r], ksem.at[r]).start()
        pltpu.make_async_copy(cv_hbm.at[r, :, 0], vbuf.at[r], vsem.at[r]).start()

    for i in range(RING):
        start_weight(jnp.int32(i))
    x_copy.wait()

    def norm_step(i, carry):
        rows = pl.ds(pl.multiple_of(i * 16, 16), 16)
        wide = x_ref[rows, :].astype(jnp.float32)
        inv = lax.rsqrt(jnp.mean(wide * wide, axis=-1, keepdims=True) + NORM_EPS)
        h_ref[rows, :] = (wide * inv * gain_ref[...].astype(jnp.float32)).astype(jnp.bfloat16)
        return carry

    lax.fori_loop(0, ROWS // 16, norm_step, 0)

    def proj_step(i, carry):
        slot = lax.rem(i, RING)
        pltpu.make_async_copy(wk_hbm, wbuf.at[slot], wsem.at[slot]).wait()
        acc = jnp.dot(h_ref[...], wbuf[slot], preferred_element_type=jnp.float32)
        for hh in range(TILE // HEAD):
            part = acc[:, hh * HEAD:(hh + 1) * HEAD]
            turned = pltpu.roll(part, HEAD // 2, 1)
            cos_tab = jnp.where(i < NTILE - 1, cos_ref[...], 1.0)
            sin_tab = jnp.where(i < NTILE - 1, sin_ref[...], 0.0)
            qkv[(TILE // HEAD) * i + hh] = part * cos_tab + turned * sin_tab

        @pl.when(i + RING < NTILE)
        def _():
            start_weight(i + RING)

        @pl.when(i + RING >= NTILE)
        def _():
            start_cache(i + RING - NTILE)
        return carry

    lax.fori_loop(0, NTILE, proj_step, 0)

    def attend_step(r, carry):
        @pl.when(r + RING < REQ)
        def _():
            start_cache(r + RING)

        pltpu.make_async_copy(ck_hbm.at[r, :, 0], kbuf.at[r], ksem.at[r]).wait()
        pltpu.make_async_copy(cv_hbm.at[r, :, 0], vbuf.at[r], vsem.at[r]).wait()
        ctx = ctx_ref[r]
        rows = pl.ds(pl.multiple_of(r * TREE, 8), TREE)
        first = ctx // BLK
        last = (ctx + TREE - 1) // BLK

        def insert(block):
            j = block // CP
            slot_of = lax.broadcasted_iota(jnp.int32, (BLK, TREE), 0) + (block * BLK - ctx)
            pick = (slot_of == lax.broadcasted_iota(jnp.int32, (BLK, TREE), 1)).astype(jnp.bfloat16)
            wide_slot = lax.broadcasted_iota(jnp.int32, (BLK, HEAD), 0) + (block * BLK - ctx)
            inside = (wide_slot >= 0) & (wide_slot < TREE)
            for hd in range(KV):
                for buf, base in ((kbuf, HEADS), (vbuf, HEADS + KV)):
                    new = qkv[base + hd, rows, :].astype(jnp.bfloat16)
                    placed = jnp.dot(pick, new, preferred_element_type=jnp.float32)
                    old = buf[r, j, hd].astype(jnp.float32)
                    buf[r, j, hd] = jnp.where(inside, placed, old).astype(jnp.bfloat16)

        @pl.when(lax.rem(first, CP) == cp_rank)
        def _():
            insert(first)

        @pl.when((lax.rem(last, CP) == cp_rank) & (last != first))
        def _():
            insert(last)

        pltpu.make_async_copy(kbuf.at[r], nk_hbm.at[r, :, 0], nksem.at[r]).start()
        pltpu.make_async_copy(vbuf.at[r], nv_hbm.at[r, :, 0], nvsem.at[r]).start()

        lane = lax.broadcasted_iota(jnp.int32, (TREE, NBLK * BLK), 1)
        pos = (lane // BLK * CP + cp_rank) * BLK + lane % BLK - ctx
        onehot = (pos == lax.broadcasted_iota(jnp.int32, (TREE, NBLK * BLK), 0)).astype(jnp.bfloat16)
        allowed = jnp.dot(mask_ref[r].astype(jnp.float32).astype(jnp.bfloat16), onehot, preferred_element_type=jnp.float32)
        bias = jnp.where((pos < 0) | (allowed > 0.5), 0.0, MASKED)

        stats = jnp.zeros((TREE, HEAD), jnp.float32)
        stat_lane = lax.broadcasted_iota(jnp.int32, (TREE, HEAD), 1)
        for hd in range(KV):
            query = qkv[hd * GROUP:(hd + 1) * GROUP, rows, :].reshape(GROUP * TREE, HEAD).astype(jnp.bfloat16)
            keys = kbuf[r, :, hd].reshape(NBLK * BLK, HEAD)
            vals = vbuf[r, :, hd].reshape(NBLK * BLK, HEAD)
            score = lax.dot_general(query, keys, (((1,), (1,)), ((), ())), preferred_element_type=jnp.float32)
            score = score.reshape(GROUP, TREE, NBLK * BLK) * (HEAD ** -0.5 * LOG2E) + bias[None]
            top = jnp.max(score, axis=-1, keepdims=True)
            prob = jnp.exp2(score - top)
            total = jnp.sum(prob, axis=-1, keepdims=True)
            mixed = jnp.dot(prob.reshape(GROUP * TREE, NBLK * BLK).astype(jnp.bfloat16), vals, preferred_element_type=jnp.float32)
            for g in range(GROUP):
                head = hd * GROUP + g
                obuf[r, :, head * HEAD:(head + 1) * HEAD] = mixed[g * TREE:(g + 1) * TREE]
                stats = jnp.where(stat_lane == head, top[g], stats)
                stats = jnp.where(stat_lane == HEADS + head, total[g], stats)
        obuf[r, :, WIDE:] = stats
        pltpu.make_async_copy(obuf.at[r], o_hbm.at[r], osem.at[r]).start()
        return carry

    lax.fori_loop(0, REQ, attend_step, 0)

    def drain(r, carry):
        pltpu.make_async_copy(kbuf.at[r], nk_hbm.at[r, :, 0], nksem.at[r]).wait()
        pltpu.make_async_copy(vbuf.at[r], nv_hbm.at[r, :, 0], nvsem.at[r]).wait()
        pltpu.make_async_copy(obuf.at[r], o_hbm.at[r], osem.at[r]).wait()
        return carry

    lax.fori_loop(0, REQ, drain, 0)


def merge(a, b):
    ta, tb = a[:, WIDE:], b[:, WIDE:]
    top = jnp.maximum(ta, tb)
    fa, fb = jnp.exp2(ta - top), jnp.exp2(tb - top)
    total = ta * pltpu.roll(fa, HEADS, 1) + tb * pltpu.roll(fb, HEADS, 1)
    lane = lax.broadcasted_iota(jnp.int32, (TREE, HEAD), 1)
    return fa, fb, top, total, jnp.where(lane < HEADS, top, total)


def tail_kernel(o_hbm, w_hbm, x_hbm, y_ref,
                own, pin, ysend, yrecv, keep, heads, hbf, wbuf, xbuf,
                part, in_end, in_mid, fin, fin_y, fin_c, fin_cy,
                osem, wsem, xsem, s_p, r_p, s_y, r_y, s_a, r_a,
                s_e, r_e, s_m, r_m, s_f, r_f, s_yf, r_yf, s_cf, r_cf, s_cy, r_cy):
    cp_rank = lax.axis_index('cp')
    z = lax.axis_index('tp')
    yy = cp_rank // 2
    core = cp_rank % 2
    other_core = 1 - core
    other_y = 1 - yy
    mid = (z + 1) // 2 % 2
    partner = {'cp': yy * 2 + other_core}
    across = {'cp': other_y * 2 + core}
    pair = {'tp': z + 1 - 2 * (z % 2)}
    middle = {'tp': 3 - z}

    def remote(src, dst, send, recv, peer):
        return pltpu.make_async_remote_copy(src_ref=src, dst_ref=dst, send_sem=send, recv_sem=recv, device_id=peer, device_id_type=MESH)

    own_copies = [pltpu.make_async_copy(o_hbm.at[r], own.at[r], osem.at[r]) for r in range(REQ)]
    for copy in own_copies:
        copy.start()

    def weight_copy(j):
        cols = pl.ds(pl.multiple_of(core * HALF + j * W, W), W)
        return pltpu.make_async_copy(w_hbm.at[:, cols], wbuf.at[j], wsem.at[j])

    def start_weight(j, carry):
        weight_copy(j).start()
        return carry

    lax.fori_loop(0, NP, start_weight, 0)
    x_copy = pltpu.make_async_copy(
        x_hbm.at[pl.ds(pl.multiple_of(yy * MINE, 16), MINE), pl.ds(pl.multiple_of(core * HALF, HALF), HALF)], xbuf, xsem)
    x_copy.start()

    barrier = pltpu.get_barrier_semaphore()
    for peer in (partner, across, pair):
        pl.semaphore_signal(barrier, inc=1, device_id=peer, device_id_type=MESH)

    @pl.when(mid == 1)
    def _():
        pl.semaphore_signal(barrier, inc=1, device_id=middle, device_id_type=MESH)
        pl.semaphore_wait(barrier, 4)

    @pl.when(mid == 0)
    def _():
        pl.semaphore_wait(barrier, 3)

    for copy in own_copies:
        copy.wait()

    def chip_copy(side, q):
        chip = yy if side else other_y
        return remote(own.at[6 * chip + 3 * other_core + q], pin.at[3 * side + q], s_p.at[3 * side + q], r_p.at[3 * side + q], partner)

    for side in (0, 1):
        for q in range(3):
            chip_copy(side, q).start()

    def y_copy(q):
        return remote(ysend.at[q], yrecv.at[q], s_y.at[q], r_y.at[q], across)

    def blend(a, b, out):
        fa, fb, top, total, stats = merge(a, b)
        for h in range(HEADS):
            cols = slice(h * HEAD, (h + 1) * HEAD)
            out[:, cols] = a[:, cols] * fa[:, h:h + 1] + b[:, cols] * fb[:, h:h + 1]
        out[:, WIDE:] = stats

    for q in range(3):
        chip_copy(0, q).wait_recv()
        blend(own.at[6 * other_y + 3 * core + q], pin.at[q], ysend.at[q])
        y_copy(q).start()
    for q in range(3):
        chip_copy(1, q).wait_recv()
        blend(own.at[6 * yy + 3 * core + q], pin.at[3 + q], keep.at[q])

    def head_copy(q, owner):
        slot = 3 * owner + q
        return remote(heads.at[slot], heads.at[slot], s_a.at[q], r_a.at[q], partner)

    for q in range(3):
        y_copy(q).wait_recv()
        a, b, out = keep.at[q], yrecv.at[q], heads.at[3 * core + q]
        fa, fb, top, total, stats = merge(a, b)
        inv = 1.0 / total
        for h in range(HEADS):
            cols = slice(h * HEAD, (h + 1) * HEAD)
            mixed = a[:, cols] * fa[:, h:h + 1] + b[:, cols] * fb[:, h:h + 1]
            out[:, cols] = mixed * inv[:, HEADS + h:HEADS + h + 1]
        head_copy(q, core).start()
    for q in range(3):
        head_copy(q, other_core).wait_recv()
    hbf[...] = heads[...].reshape(MINE, WIDE).astype(jnp.bfloat16)

    def end_copy(j):
        return remote(part.at[j], in_end.at[j], s_e.at[j], r_e.at[j], pair)

    def mid_copy(j):
        return remote(part.at[j], in_mid.at[j], s_m.at[j], r_m.at[j], middle)

    def fin_copy(j):
        return remote(fin.at[j], fin.at[j], s_f.at[j], r_f.at[j], pair)

    def across_copy(j):
        return remote(fin.at[j], fin_y.at[j], s_yf.at[j], r_yf.at[j], across)

    def core_copy(j):
        return remote(fin.at[j], fin_c.at[j], s_cf.at[j], r_cf.at[j], partner)

    def core_y_copy(j):
        return remote(fin_y.at[j], fin_cy.at[j], s_cy.at[j], r_cy.at[j], partner)

    def project(j, carry):
        weight_copy(j).wait()
        prod = jnp.dot(hbf[...], wbuf[j], preferred_element_type=jnp.float32)
        part[j] = prod.astype(jnp.bfloat16).astype(jnp.float32)

        @pl.when(mid == 0)
        def _():
            end_copy(j).start()
        return carry

    lax.fori_loop(0, NP, project, 0)
    x_copy.wait()

    def emit(buf, j, chip, half):
        rows = pl.ds(pl.multiple_of(chip * MINE, 16), MINE)
        cols = pl.ds(pl.multiple_of(half * HALF + j * W, W), W)
        y_ref[rows, cols] = buf[j].astype(jnp.bfloat16)

    def staged(s, lag, body):
        j = s - lag

        @pl.when((j >= 0) & (j < NP))
        def _():
            body(j)

    def take_end(j):
        end_copy(j).wait_recv()
        part[j] = part[j] + in_end[j]
        mid_copy(j).start()

    def take_mid(j):
        mid_copy(j).wait_recv()
        xcols = pl.ds(pl.multiple_of(j * W, W), W)
        fin[j] = (part[j] + in_mid[j]) + xbuf[:, xcols].astype(jnp.float32)
        fin_copy(j).start()
        across_copy(j).start()
        core_copy(j).start()
        emit(fin, j, yy, core)

    def take_fin(j):
        fin_copy(j).wait_recv()
        across_copy(j).start()
        core_copy(j).start()
        emit(fin, j, yy, core)

    def take_core(j):
        core_copy(j).wait_recv()
        emit(fin_c, j, yy, other_core)

    def take_across(j):
        across_copy(j).wait_recv()
        core_y_copy(j).start()
        emit(fin_y, j, other_y, core)

    def take_core_y(j):
        core_y_copy(j).wait_recv()
        emit(fin_cy, j, other_y, other_core)

    @pl.when(mid == 1)
    def _():
        def step(s, carry):
            staged(s, 0, take_end)
            staged(s, 1, take_mid)
            staged(s, 2, take_core)
            staged(s, 4, take_across)
            staged(s, 5, take_core_y)
            return carry

        lax.fori_loop(0, NP + 5, step, 0)

    @pl.when(mid == 0)
    def _():
        def step(s, carry):
            staged(s, 0, take_fin)
            staged(s, 1, take_core)
            staged(s, 2, take_across)
            staged(s, 3, take_core_y)
            return carry

        lax.fori_loop(0, NP + 3, step, 0)

    for side in (0, 1):
        for q in range(3):
            chip_copy(side, q).wait_send()
    for q in range(3):
        y_copy(q).wait_send()
        head_copy(q, core).wait_send()

    def sent(j, carry):
        across_copy(j).wait_send()
        core_copy(j).wait_send()
        core_y_copy(j).wait_send()

        @pl.when(mid == 1)
        def _():
            mid_copy(j).wait_send()
            fin_copy(j).wait_send()

        @pl.when(mid == 0)
        def _():
            end_copy(j).wait_send()
        return carry

    lax.fori_loop(0, NP, sent, 0)


def solution(mesh):
    cache_spec = P('dp', None, 'cp', 'tp')
    row_spec = P('dp')
    anywhere = pl.BlockSpec(memory_space=pl.ANY)
    vmem = pl.BlockSpec(memory_space=pltpu.VMEM)
    smem = pl.BlockSpec(memory_space=pltpu.SMEM)
    dma = pltpu.SemaphoreType.DMA
    f32, bf16 = jnp.float32, jnp.bfloat16

    def local_step(hidden, attn_gain, w_query, w_key, w_value, w_out, cache_k, cache_v, ctx_len, positions, tree_mask):
        cos_tab, sin_tab = rope_tables(positions)
        flat = hidden.reshape(ROWS, D)
        cache_shape = jax.ShapeDtypeStruct(cache_k.shape, bf16)
        partial_out, new_k, new_v = pl.pallas_call(
            attend_kernel,
            out_shape=(jax.ShapeDtypeStruct((REQ, TREE, EXT), f32), cache_shape, cache_shape),
            in_specs=[smem, vmem, vmem, vmem, vmem] + [anywhere] * 6,
            out_specs=(anywhere, anywhere, anywhere),
            scratch_shapes=[
                pltpu.VMEM((ROWS, D), bf16), pltpu.VMEM((ROWS, D), bf16), pltpu.VMEM((RING, D, TILE), bf16),
                pltpu.VMEM((HEADS + 2 * KV, ROWS, HEAD), f32),
                pltpu.VMEM((REQ, NBLK, KV, BLK, HEAD), bf16), pltpu.VMEM((REQ, NBLK, KV, BLK, HEAD), bf16),
                pltpu.VMEM((REQ, TREE, EXT), f32),
                dma, dma((RING,)), dma((REQ,)), dma((REQ,)), dma((REQ,)), dma((REQ,)), dma((REQ,)),
            ],
            compiler_params=pltpu.CompilerParams(vmem_limit_bytes=62 * 1024 * 1024),
            cost_estimate=pl.CostEstimate(flops=20_000_000_000, bytes_accessed=72_000_000, transcendentals=5_000_000),
            name='attend',
        )(ctx_len, attn_gain.reshape(1, D), cos_tab, sin_tab, tree_mask, flat, w_query, w_key, w_value, cache_k, cache_v)
        pieces = pltpu.VMEM((NP, MINE, W), f32)
        out = pl.pallas_call(
            tail_kernel,
            out_shape=jax.ShapeDtypeStruct((ROWS, D), bf16),
            in_specs=[anywhere] * 3,
            out_specs=vmem,
            scratch_shapes=[
                pltpu.VMEM((REQ, TREE, EXT), f32), pltpu.VMEM((6, TREE, EXT), f32), pltpu.VMEM((3, TREE, EXT), f32),
                pltpu.VMEM((3, TREE, EXT), f32), pltpu.VMEM((3, TREE, EXT), f32), pltpu.VMEM((6, TREE, WIDE), f32),
                pltpu.VMEM((MINE, WIDE), bf16), pltpu.VMEM((NP, WIDE, W), bf16), pltpu.VMEM((MINE, HALF), bf16),
                pieces, pieces, pieces, pieces, pieces, pieces, pieces,
                dma((REQ,)), dma((NP,)), dma, dma((6,)), dma((6,)), dma((3,)), dma((3,)), dma((3,)), dma((3,)),
            ] + [dma((NP,)) for _ in range(12)],
            compiler_params=pltpu.CompilerParams(vmem_limit_bytes=62 * 1024 * 1024, collective_id=0, has_side_effects=True),
            cost_estimate=pl.CostEstimate(flops=2_500_000_000, bytes_accessed=30_000_000, transcendentals=100_000),
            name='tail',
        )(partial_out, w_out, flat)
        return out.reshape(REQ, TREE, D), new_k, new_v

    return jax.shard_map(local_step, mesh=mesh, in_specs=(row_spec, P(), P(None, 'tp'), P(None, 'tp'), P(None, 'tp'), P('tp', None), cache_spec, cache_spec, row_spec, row_spec, row_spec), out_specs=(row_spec, cache_spec, cache_spec), check_vma=False)
```

```python
import math
import jax
import jax.numpy as jnp
from jax import lax
from jax.experimental import pallas as pl
from jax.experimental.pallas import tpu as pltpu
from jax.sharding import PartitionSpec as P

ROPE_THETA = 500000.0
NORM_EPS = 1e-5
MASKED = -1e30
LOG2E = 1.4426950408889634
MESH = pl.DeviceIdType.MESH

REQ = 12
TREE = 24
ROWS = REQ * TREE
D = 8192
HEAD = 128
KV = 2
GROUP = 8
HEADS = KV * GROUP
NBLK = 4
BLK = 256
CP = 4
WIDE = HEADS * HEAD
EXT = WIDE + HEAD
TILE = 256
NTILE = (HEADS + 2 * KV) * HEAD // TILE
RING = 4
HALF = D // 2
NP = 16
W = HALF // NP
WAVES = 3
WAVE_ROWS = CP * TREE
PART_ROWS = WAVE_ROWS // 2
PIECES = WAVES * NP
AHEAD = 8


def rope_tables(positions):
    freq_idx = jnp.arange(HEAD // 2, dtype=jnp.float32)
    inv_freq = 1.0 / (ROPE_THETA ** (2.0 * freq_idx / HEAD))
    wavelen = 2.0 * math.pi / inv_freq
    smooth = (8192.0 / wavelen - 1.0) / 3.0
    blended = (1.0 - smooth) * inv_freq / 8.0 + smooth * inv_freq
    inv_freq = jnp.where(wavelen < 2048.0, inv_freq, jnp.where(wavelen > 8192.0, inv_freq / 8.0, blended))
    angle = positions.astype(jnp.float32)[..., None] * inv_freq
    return jnp.cos(angle).reshape(ROWS, HEAD // 2), jnp.sin(angle).reshape(ROWS, HEAD // 2)


def attend_kernel(ctx_ref, gain_ref, cos_ref, sin_ref, mask_ref, x_hbm, wq_hbm, wk_hbm, wv_hbm, ck_hbm, cv_hbm,
                  o_ref, nk_hbm, nv_hbm,
                  x_ref, h_ref, turn, wbuf, qkv, kbuf, vbuf, xsem, wsem, ksem, vsem, nksem, nvsem):
    cp_rank = lax.axis_index('cp')
    nq = HEADS * HEAD // TILE

    x_copy = pltpu.make_async_copy(x_hbm, x_ref, xsem)
    x_copy.start()

    def start_weight(i):
        slot = lax.rem(i, RING)

        @pl.when(i < nq)
        def _():
            cols = pl.ds(pl.multiple_of(i * TILE, TILE), TILE)
            pltpu.make_async_copy(wq_hbm.at[:, cols], wbuf.at[slot], wsem.at[slot]).start()

        @pl.when(i == nq)
        def _():
            pltpu.make_async_copy(wk_hbm, wbuf.at[slot], wsem.at[slot]).start()

        @pl.when(i == nq + 1)
        def _():
            pltpu.make_async_copy(wv_hbm, wbuf.at[slot], wsem.at[slot]).start()

    def start_cache(r):
        pltpu.make_async_copy(ck_hbm.at[r, :, 0], kbuf.at[r], ksem.at[r]).start()
        pltpu.make_async_copy(cv_hbm.at[r, :, 0], vbuf.at[r], vsem.at[r]).start()

    for i in range(RING):
        start_weight(jnp.int32(i))
    turn[0] = jnp.concatenate([cos_ref[...], cos_ref[...]], axis=-1)
    turn[1] = jnp.concatenate([-sin_ref[...], sin_ref[...]], axis=-1)
    x_copy.wait()

    def norm_step(i, carry):
        rows = pl.ds(pl.multiple_of(i * 16, 16), 16)
        squares = [jnp.zeros((16, HEAD), jnp.float32) for _ in range(2)]
        for k in range(D // HEAD):
            wide = x_ref[rows, k * HEAD:(k + 1) * HEAD].astype(jnp.float32)
            squares[k % 2] = squares[k % 2] + wide * wide
        inv = lax.rsqrt(jnp.sum(squares[0] + squares[1], axis=-1, keepdims=True) * (1.0 / D) + NORM_EPS)
        for k in range(D // HEAD):
            cols = slice(k * HEAD, (k + 1) * HEAD)
            wide = x_ref[rows, cols].astype(jnp.float32)
            h_ref[rows, cols] = (wide * inv * gain_ref[cols].astype(jnp.float32).reshape(1, HEAD)).astype(jnp.bfloat16)
        return carry

    lax.fori_loop(0, ROWS // 16, norm_step, 0)

    def proj_step(i, carry):
        slot = lax.rem(i, RING)
        pltpu.make_async_copy(wk_hbm, wbuf.at[slot], wsem.at[slot]).wait()
        acc = jnp.dot(h_ref[...], wbuf[slot], preferred_element_type=jnp.float32)
        for hh in range(TILE // HEAD):
            part = acc[:, hh * HEAD:(hh + 1) * HEAD]
            turned = pltpu.roll(part, HEAD // 2, 1)
            cos_tab = jnp.where(i < NTILE - 1, turn[0], 1.0)
            sin_tab = jnp.where(i < NTILE - 1, turn[1], 0.0)
            qkv[(TILE // HEAD) * i + hh] = part * cos_tab + turned * sin_tab

        @pl.when(i + RING < NTILE)
        def _():
            start_weight(i + RING)

        @pl.when(i + RING >= NTILE)
        def _():
            start_cache(i + RING - NTILE)
        return carry

    lax.fori_loop(0, NTILE, proj_step, 0)

    def attend_step(r, carry):
        @pl.when(r + RING < REQ)
        def _():
            start_cache(r + RING)

        pltpu.make_async_copy(ck_hbm.at[r, :, 0], kbuf.at[r], ksem.at[r]).wait()
        pltpu.make_async_copy(cv_hbm.at[r, :, 0], vbuf.at[r], vsem.at[r]).wait()
        ctx = ctx_ref[r]
        rows = pl.ds(pl.multiple_of(r * TREE, 8), TREE)
        first = ctx // BLK
        last = (ctx + TREE - 1) // BLK

        def insert(block):
            j = block // CP
            slot_of = lax.broadcasted_iota(jnp.int32, (BLK, TREE), 0) + (block * BLK - ctx)
            pick = (slot_of == lax.broadcasted_iota(jnp.int32, (BLK, TREE), 1)).astype(jnp.bfloat16)
            wide_slot = lax.broadcasted_iota(jnp.int32, (BLK, HEAD), 0) + (block * BLK - ctx)
            inside = (wide_slot >= 0) & (wide_slot < TREE)
            for hd in range(KV):
                for buf, base in ((kbuf, HEADS), (vbuf, HEADS + KV)):
                    new = qkv[base + hd, rows, :].astype(jnp.bfloat16)
                    placed = jnp.dot(pick, new, preferred_element_type=jnp.float32)
                    old = buf[r, j, hd].astype(jnp.float32)
                    buf[r, j, hd] = jnp.where(inside, placed, old).astype(jnp.bfloat16)

        @pl.when(lax.rem(first, CP) == cp_rank)
        def _():
            insert(first)

        @pl.when((lax.rem(last, CP) == cp_rank) & (last != first))
        def _():
            insert(last)

        pltpu.make_async_copy(kbuf.at[r], nk_hbm.at[r, :, 0], nksem.at[r]).start()
        pltpu.make_async_copy(vbuf.at[r], nv_hbm.at[r, :, 0], nvsem.at[r]).start()

        lane = lax.broadcasted_iota(jnp.int32, (TREE, NBLK * BLK), 1)
        pos = (lane // BLK * CP + cp_rank) * BLK + lane % BLK - ctx
        onehot = (pos == lax.broadcasted_iota(jnp.int32, (TREE, NBLK * BLK), 0)).astype(jnp.bfloat16)
        allowed = jnp.dot(mask_ref[r].astype(jnp.float32).astype(jnp.bfloat16), onehot, preferred_element_type=jnp.float32)
        bias = jnp.where((pos < 0) | (allowed > 0.5), 0.0, MASKED)

        stats = jnp.zeros((TREE, HEAD), jnp.float32)
        stat_lane = lax.broadcasted_iota(jnp.int32, (TREE, HEAD), 1)
        for hd in range(KV):
            query = qkv[hd * GROUP:(hd + 1) * GROUP, rows, :].reshape(GROUP * TREE, HEAD).astype(jnp.bfloat16)
            keys = kbuf[r, :, hd].reshape(NBLK * BLK, HEAD)
            vals = vbuf[r, :, hd].reshape(NBLK * BLK, HEAD)
            score = lax.dot_general(query, keys, (((1,), (1,)), ((), ())), preferred_element_type=jnp.float32)
            score = score.reshape(GROUP, TREE, NBLK * BLK) * (HEAD ** -0.5 * LOG2E) + bias[None]
            top = jnp.max(score, axis=-1, keepdims=True)
            prob = jnp.exp2(score - top)
            total = jnp.sum(prob, axis=-1, keepdims=True)
            mixed = jnp.dot(prob.reshape(GROUP * TREE, NBLK * BLK).astype(jnp.bfloat16), vals, preferred_element_type=jnp.float32)
            for g in range(GROUP):
                head = hd * GROUP + g
                o_ref[r, :, head * HEAD:(head + 1) * HEAD] = mixed[g * TREE:(g + 1) * TREE]
                stats = jnp.where(stat_lane == head, top[g], stats)
                stats = jnp.where(stat_lane == HEADS + head, total[g], stats)
        o_ref[r, :, WIDE:] = stats
        return carry

    lax.fori_loop(0, REQ, attend_step, 0)

    def drain(r, carry):
        pltpu.make_async_copy(kbuf.at[r], nk_hbm.at[r, :, 0], nksem.at[r]).wait()
        pltpu.make_async_copy(vbuf.at[r], nv_hbm.at[r, :, 0], nvsem.at[r]).wait()
        return carry

    lax.fori_loop(0, REQ, drain, 0)


def merge(a, b):
    ta, tb = a[:, WIDE:], b[:, WIDE:]
    top = jnp.maximum(ta, tb)
    fa, fb = jnp.exp2(ta - top), jnp.exp2(tb - top)
    total = ta * pltpu.roll(fa, HEADS, 1) + tb * pltpu.roll(fb, HEADS, 1)
    lane = lax.broadcasted_iota(jnp.int32, (TREE, HEAD), 1)
    return fa, fb, total, jnp.where(lane < HEADS, top, total)


def tail_kernel(own, w_hbm, x_hbm, y_ref,
                pin, yrecv, heads, hbf, wbuf, xbuf,
                part, in_end, in_mid, fin, fin_y, fin_c, fin_cy,
                wsem, xsem, s_p, r_p, s_y, r_y, s_a, r_a,
                s_e, r_e, s_m, r_m, s_f, r_f, s_yf, r_yf, s_cf, r_cf, s_cy, r_cy):
    cp_rank = lax.axis_index('cp')
    z = lax.axis_index('tp')
    yy = cp_rank // 2
    core = cp_rank % 2
    other_core = 1 - core
    other_y = 1 - yy
    mid = (z + 1) // 2 % 2
    partner = {'cp': yy * 2 + other_core}
    across = {'cp': other_y * 2 + core}
    pair = {'tp': z + 1 - 2 * (z % 2)}
    middle = {'tp': 3 - z}

    def remote(src, dst, send, recv, peer):
        return pltpu.make_async_remote_copy(src_ref=src, dst_ref=dst, send_sem=send, recv_sem=recv, device_id=peer, device_id_type=MESH)

    barrier = pltpu.get_barrier_semaphore()
    for peer in (partner, across, pair):
        pl.semaphore_signal(barrier, inc=1, device_id=peer, device_id_type=MESH)

    @pl.when(mid == 1)
    def _():
        pl.semaphore_signal(barrier, inc=1, device_id=middle, device_id_type=MESH)

    def weight_copy(j):
        cols = pl.ds(pl.multiple_of(core * HALF + j * W, W), W)
        return pltpu.make_async_copy(w_hbm.at[:, cols], wbuf.at[j], wsem.at[j])

    def start_weight(j, carry):
        weight_copy(j).start()
        return carry

    lax.fori_loop(0, NP, start_weight, 0)
    x_copies = [pltpu.make_async_copy(
        x_hbm.at[pl.ds(pl.multiple_of(w * WAVE_ROWS + yy * PART_ROWS, 16), PART_ROWS), pl.ds(pl.multiple_of(core * HALF, HALF), HALF)],
        xbuf.at[w], xsem.at[w]) for w in range(WAVES)]
    for copy in x_copies:
        copy.start()

    @pl.when(mid == 1)
    def _():
        pl.semaphore_wait(barrier, 4)

    @pl.when(mid == 0)
    def _():
        pl.semaphore_wait(barrier, 3)

    def chip_copy(w, side):
        chip = yy if side else other_y
        return remote(own.at[4 * w + 2 * chip + other_core], pin.at[w, side], s_p.at[w, side], r_p.at[w, side], partner)

    for w in range(WAVES):
        for side in (0, 1):
            chip_copy(w, side).start()

    def y_copy(w):
        return remote(pin.at[w, 0], yrecv.at[w], s_y.at[w], r_y.at[w], across)

    def blend(a, b):
        fa, fb, total, stats = merge(a, b)
        for h in range(HEADS):
            cols = slice(h * HEAD, (h + 1) * HEAD)
            b[:, cols] = a[:, cols] * fa[:, h:h + 1] + b[:, cols] * fb[:, h:h + 1]
        b[:, WIDE:] = stats

    def head_copy(w, owner):
        return remote(heads.at[w, owner], heads.at[w, owner], s_a.at[w], r_a.at[w], partner)

    def finish_start(w):
        y_copy(w).wait_recv()
        a, b, out = pin.at[w, 1], yrecv.at[w], heads.at[w, core]
        fa, fb, total, stats = merge(a, b)
        inv = 1.0 / total
        for h in range(HEADS):
            cols = slice(h * HEAD, (h + 1) * HEAD)
            mixed = a[:, cols] * fa[:, h:h + 1] + b[:, cols] * fb[:, h:h + 1]
            out[:, cols] = mixed * inv[:, HEADS + h:HEADS + h + 1]
        head_copy(w, core).start()

    def finish_end(w):
        head_copy(w, other_core).wait_recv()
        hbf[...] = heads[w].reshape(PART_ROWS, WIDE).astype(jnp.bfloat16)

    for w in range(WAVES):
        chip_copy(w, 0).wait_recv()
        blend(own.at[4 * w + 2 * other_y + core], pin.at[w, 0])
        y_copy(w).start()
    for w in range(WAVES):
        chip_copy(w, 1).wait_recv()
        blend(own.at[4 * w + 2 * yy + core], pin.at[w, 1])
    for copy in x_copies:
        copy.wait()
    finish_start(0)
    finish_end(0)

    def end_copy(p):
        return remote(part.at[p], in_end.at[p], s_e.at[p], r_e.at[p], pair)

    def mid_copy(p):
        return remote(part.at[p], in_mid.at[p], s_m.at[p], r_m.at[p], middle)

    def fin_copy(p):
        return remote(fin.at[p], fin.at[p], s_f.at[p], r_f.at[p], pair)

    def across_copy(p):
        return remote(fin.at[p], fin_y.at[p], s_yf.at[p], r_yf.at[p], across)

    def core_copy(p):
        return remote(fin.at[p], fin_c.at[p], s_cf.at[p], r_cf.at[p], partner)

    def core_y_copy(p):
        return remote(fin_y.at[p], fin_cy.at[p], s_cy.at[p], r_cy.at[p], partner)

    def project(p):
        j = p % NP

        @pl.when(p < NP)
        def _():
            weight_copy(j).wait()

        prod = jnp.dot(hbf[...], wbuf[j], preferred_element_type=jnp.float32)
        part[p] = prod.astype(jnp.bfloat16).astype(jnp.float32)

        @pl.when(mid == 0)
        def _():
            end_copy(p).start()

    def emit(buf, p, chip, half):
        rows = pl.ds(pl.multiple_of(p // NP * WAVE_ROWS + chip * PART_ROWS, 16), PART_ROWS)
        cols = pl.ds(pl.multiple_of(half * HALF + p % NP * W, W), W)
        y_ref[rows, cols] = buf[p].astype(jnp.bfloat16)

    def take_end(p):
        end_copy(p).wait_recv()
        part[p] = part[p] + in_end[p]
        mid_copy(p).start()

    def take_mid(p):
        mid_copy(p).wait_recv()
        xcols = pl.ds(pl.multiple_of(p % NP * W, W), W)
        fin[p] = (part[p] + in_mid[p]) + xbuf[p // NP, :, xcols].astype(jnp.float32)
        fin_copy(p).start()
        across_copy(p).start()
        core_copy(p).start()
        emit(fin, p, yy, core)

    def take_fin(p):
        fin_copy(p).wait_recv()
        across_copy(p).start()
        core_copy(p).start()
        emit(fin, p, yy, core)

    def take_core(p):
        core_copy(p).wait_recv()
        emit(fin_c, p, yy, other_core)

    def take_across(p):
        across_copy(p).wait_recv()
        core_y_copy(p).start()
        emit(fin_y, p, other_y, core)

    def take_core_y(p):
        core_y_copy(p).wait_recv()
        emit(fin_cy, p, other_y, other_core)

    def ahead_step(p, carry):
        project(p)
        return carry

    lax.fori_loop(0, AHEAD, ahead_step, 0)
    lag = lambda at_mid, at_end: jnp.where(mid == 1, at_mid, at_end)
    lag_core, lag_across, lag_core_y = lag(6, 9), lag(8, 11), lag(10, 13)

    def step(s, carry):
        for w in range(1, WAVES):
            @pl.when(s == w * NP - AHEAD - 4)
            def _():
                finish_start(w)

            @pl.when(s == w * NP - AHEAD)
            def _():
                finish_end(w)

        @pl.when(s + AHEAD < PIECES)
        def _():
            project(s + AHEAD)

        @pl.when((mid == 1) & (s < PIECES))
        def _():
            take_end(s)

        @pl.when((mid == 1) & (s >= 4) & (s < PIECES + 4))
        def _():
            take_mid(s - 4)

        @pl.when((mid == 0) & (s >= 7) & (s < PIECES + 7))
        def _():
            take_fin(s - 7)

        for this_lag, body in ((lag_core, take_core), (lag_across, take_across), (lag_core_y, take_core_y)):
            p = s - this_lag

            @pl.when((p >= 0) & (p < PIECES))
            def _():
                body(p)
        return carry

    lax.fori_loop(0, PIECES + 13, step, 0)

    for w in range(WAVES):
        for side in (0, 1):
            chip_copy(w, side).wait_send()
        y_copy(w).wait_send()
        head_copy(w, core).wait_send()

    def sent(p, carry):
        across_copy(p).wait_send()
        core_copy(p).wait_send()
        core_y_copy(p).wait_send()

        @pl.when(mid == 1)
        def _():
            mid_copy(p).wait_send()
            fin_copy(p).wait_send()

        @pl.when(mid == 0)
        def _():
            end_copy(p).wait_send()
        return carry

    lax.fori_loop(0, PIECES, sent, 0)


def solution(mesh):
    cache_spec = P('dp', None, 'cp', 'tp')
    row_spec = P('dp')
    anywhere = pl.BlockSpec(memory_space=pl.ANY)
    vmem = pl.BlockSpec(memory_space=pltpu.VMEM)
    smem = pl.BlockSpec(memory_space=pltpu.SMEM)
    dma = pltpu.SemaphoreType.DMA
    f32, bf16 = jnp.float32, jnp.bfloat16

    def local_step(hidden, attn_gain, w_query, w_key, w_value, w_out, cache_k, cache_v, ctx_len, positions, tree_mask):
        cos_tab, sin_tab = rope_tables(positions)
        flat = hidden.reshape(ROWS, D)
        cache_shape = jax.ShapeDtypeStruct(cache_k.shape, bf16)
        partial_out, new_k, new_v = pl.pallas_call(
            attend_kernel,
            out_shape=(pltpu.VMEM((REQ, TREE, EXT), f32), cache_shape, cache_shape),
            in_specs=[smem, vmem, vmem, vmem, vmem] + [anywhere] * 6,
            out_specs=(vmem, anywhere, anywhere),
            scratch_shapes=[
                pltpu.VMEM((ROWS, D), bf16), pltpu.VMEM((ROWS, D), bf16), pltpu.VMEM((2, ROWS, HEAD), f32), pltpu.VMEM((RING, D, TILE), bf16),
                pltpu.VMEM((HEADS + 2 * KV, ROWS, HEAD), f32),
                pltpu.VMEM((REQ, NBLK, KV, BLK, HEAD), bf16), pltpu.VMEM((REQ, NBLK, KV, BLK, HEAD), bf16),
                dma, dma((RING,)), dma((REQ,)), dma((REQ,)), dma((REQ,)), dma((REQ,)),
            ],
            compiler_params=pltpu.CompilerParams(vmem_limit_bytes=56 * 1024 * 1024),
            cost_estimate=pl.CostEstimate(flops=20_000_000_000, bytes_accessed=72_000_000, transcendentals=5_000_000),
            name='attend',
        )(ctx_len, attn_gain, pltpu.with_memory_space_constraint(cos_tab, pltpu.VMEM), pltpu.with_memory_space_constraint(sin_tab, pltpu.VMEM), tree_mask, flat, w_query, w_key, w_value, cache_k, cache_v)
        pieces = pltpu.VMEM((PIECES, PART_ROWS, W), f32)
        out = pl.pallas_call(
            tail_kernel,
            out_shape=pltpu.VMEM((ROWS, D), bf16),
            in_specs=[vmem, anywhere, anywhere],
            out_specs=vmem,
            scratch_shapes=[
                pltpu.VMEM((WAVES, 2, TREE, EXT), f32), pltpu.VMEM((WAVES, TREE, EXT), f32), pltpu.VMEM((WAVES, 2, TREE, WIDE), f32),
                pltpu.VMEM((PART_ROWS, WIDE), bf16), pltpu.VMEM((NP, WIDE, W), bf16), pltpu.VMEM((WAVES, PART_ROWS, HALF), bf16),
                pieces, pieces, pieces, pieces, pieces, pieces, pieces,
                dma((NP,)), dma((WAVES,)), dma((WAVES, 2)), dma((WAVES, 2)), dma((WAVES,)), dma((WAVES,)), dma((WAVES,)), dma((WAVES,)),
            ] + [dma((PIECES,)) for _ in range(12)],
            compiler_params=pltpu.CompilerParams(vmem_limit_bytes=48 * 1024 * 1024, collective_id=0, has_side_effects=True),
            cost_estimate=pl.CostEstimate(flops=2_500_000_000, bytes_accessed=30_000_000, transcendentals=100_000),
            name='tail',
        )(pltpu.with_memory_space_constraint(partial_out, pltpu.VMEM), w_out, flat)
        return out.reshape(REQ, TREE, D), new_k, new_v

    return jax.shard_map(local_step, mesh=mesh, in_specs=(row_spec, P(), P(None, 'tp'), P(None, 'tp'), P(None, 'tp'), P('tp', None), cache_spec, cache_spec, row_spec, row_spec, row_spec), out_specs=(row_spec, cache_spec, cache_spec), check_vma=False)
```

```python
import math
import jax
import jax.numpy as jnp
from jax import lax
from jax.experimental import pallas as pl
from jax.experimental.pallas import tpu as pltpu
from jax.sharding import PartitionSpec as P

ROPE_THETA = 500000.0
NORM_EPS = 1e-5
MASKED = -1e30
UNROLL = 2
LOG2E = 1.4426950408889634
MESH = pl.DeviceIdType.MESH

REQ = 12
TREE = 24
ROWS = REQ * TREE
D = 8192
HEAD = 128
KV = 2
GROUP = 8
HEADS = KV * GROUP
NBLK = 4
BLK = 256
CP = 4
WIDE = HEADS * HEAD
EXT = WIDE + HEAD
TILE = 256
NTILE = (HEADS + 2 * KV) * HEAD // TILE
RING = 4
XCHUNKS = 3
CACHE_AHEAD = 8
EARLY = 8
LATE = REQ - EARLY
HALF = D // 2
NP = 16
W = HALF // NP
WAVES = 3
WAVE_ROWS = CP * TREE
PART_ROWS = WAVE_ROWS // 2
PIECES = WAVES * NP
AHEAD = 8


def rope_tables(positions):
    freq_idx = jnp.arange(HEAD // 2, dtype=jnp.float32)
    inv_freq = 1.0 / (ROPE_THETA ** (2.0 * freq_idx / HEAD))
    wavelen = 2.0 * math.pi / inv_freq
    smooth = (8192.0 / wavelen - 1.0) / 3.0
    blended = (1.0 - smooth) * inv_freq / 8.0 + smooth * inv_freq
    inv_freq = jnp.where(wavelen < 2048.0, inv_freq, jnp.where(wavelen > 8192.0, inv_freq / 8.0, blended))
    angle = positions.astype(jnp.float32)[..., None] * inv_freq
    return jnp.cos(angle).reshape(ROWS, HEAD // 2), jnp.sin(angle).reshape(ROWS, HEAD // 2)


def attend_kernel(ctx_ref, gain_ref, cos_ref, sin_ref, mask_ref, x_hbm, wq_hbm, wk_hbm, wv_hbm, ck_hbm, cv_hbm,
                  o_ref, qkv, nk_hbm, nv_hbm,
                  x_ref, h_ref, turn, wbuf, kbuf, vbuf, xsem, wsem, ksem, vsem, nksem, nvsem):
    cp_rank = lax.axis_index('cp')
    nq = HEADS * HEAD // TILE

    x_copies = []
    for k in range(XCHUNKS):
        rows = pl.ds(k * (ROWS // XCHUNKS), ROWS // XCHUNKS)
        x_copies.append(pltpu.make_async_copy(x_hbm.at[rows, :], x_ref.at[rows, :], xsem.at[k]))
        x_copies[k].start()

    def start_weight(i):
        slot = lax.rem(i, RING)

        @pl.when(i < nq)
        def _():
            cols = pl.ds(pl.multiple_of(i * TILE, TILE), TILE)
            pltpu.make_async_copy(wq_hbm.at[:, cols], wbuf.at[slot], wsem.at[slot]).start()

        @pl.when(i == nq)
        def _():
            pltpu.make_async_copy(wk_hbm, wbuf.at[slot], wsem.at[slot]).start()

        @pl.when(i == nq + 1)
        def _():
            pltpu.make_async_copy(wv_hbm, wbuf.at[slot], wsem.at[slot]).start()

    def start_cache(r):
        pltpu.make_async_copy(ck_hbm.at[r, :, 0], kbuf.at[r], ksem.at[r]).start()
        pltpu.make_async_copy(cv_hbm.at[r, :, 0], vbuf.at[r], vsem.at[r]).start()

    turn[0] = jnp.concatenate([cos_ref[...], cos_ref[...]], axis=-1)
    turn[1] = jnp.concatenate([-sin_ref[...], sin_ref[...]], axis=-1)
    def norm_step(i, carry):
        rows = pl.ds(pl.multiple_of(i * 16, 16), 16)
        squares = [jnp.zeros((16, HEAD), jnp.float32) for _ in range(2)]
        for k in range(D // HEAD):
            wide = x_ref[rows, k * HEAD:(k + 1) * HEAD].astype(jnp.float32)
            squares[k % 2] = squares[k % 2] + wide * wide
        inv = lax.rsqrt(jnp.sum(squares[0] + squares[1], axis=-1, keepdims=True) * (1.0 / D) + NORM_EPS)
        for k in range(D // HEAD):
            cols = slice(k * HEAD, (k + 1) * HEAD)
            wide = x_ref[rows, cols].astype(jnp.float32)
            h_ref[rows, cols] = (wide * inv * gain_ref[cols].astype(jnp.float32).reshape(1, HEAD)).astype(jnp.bfloat16)
        return carry

    for k in range(XCHUNKS):
        x_copies[k].wait()
        if k == 0:
            for i in range(RING):
                start_weight(jnp.int32(i))
        lax.fori_loop(k * (ROWS // 16 // XCHUNKS), (k + 1) * (ROWS // 16 // XCHUNKS), norm_step, 0)

    def proj_step(i, carry):
        slot = lax.rem(i, RING)
        pltpu.make_async_copy(wq_hbm.at[:, :TILE], wbuf.at[slot], wsem.at[slot]).wait()
        acc = jnp.dot(h_ref[...], wbuf[slot], preferred_element_type=jnp.float32)
        for hh in range(TILE // HEAD):
            part = acc[:, hh * HEAD:(hh + 1) * HEAD]
            turned = pltpu.roll(part, HEAD // 2, 1)
            cos_tab, sin_tab = turn[0], turn[1]
            cos_tab = jnp.where(i < NTILE - 1, cos_tab, 1.0)
            sin_tab = jnp.where(i < NTILE - 1, sin_tab, 0.0)
            qkv[(TILE // HEAD) * i + hh] = part * cos_tab + turned * sin_tab

        @pl.when(i + RING < NTILE)
        def _():
            start_weight(i + RING)

        @pl.when(i + RING >= NTILE)
        def _():
            for k in range(CACHE_AHEAD // RING):
                start_cache((i + RING - NTILE) * (CACHE_AHEAD // RING) + k)
        return carry

    lax.fori_loop(0, NTILE, proj_step, 0)

    def prepare(r):
        @pl.when(r + CACHE_AHEAD < REQ)
        def _():
            start_cache(r + CACHE_AHEAD)

        pltpu.make_async_copy(ck_hbm.at[r, :, 0], kbuf.at[r], ksem.at[r]).wait()
        pltpu.make_async_copy(cv_hbm.at[r, :, 0], vbuf.at[r], vsem.at[r]).wait()
        ctx = ctx_ref[r]
        rows = pl.ds(pl.multiple_of(r * TREE, 8), TREE)
        first = ctx // BLK
        last = (ctx + TREE - 1) // BLK

        def insert(block):
            j = block // CP
            slot_of = lax.broadcasted_iota(jnp.int32, (BLK, TREE), 0) + (block * BLK - ctx)
            pick = (slot_of == lax.broadcasted_iota(jnp.int32, (BLK, TREE), 1)).astype(jnp.bfloat16)
            wide_slot = lax.broadcasted_iota(jnp.int32, (BLK, HEAD), 0) + (block * BLK - ctx)
            inside = (wide_slot >= 0) & (wide_slot < TREE)
            for hd in range(KV):
                for buf, base in ((kbuf, HEADS), (vbuf, HEADS + KV)):
                    new = qkv[base + hd, rows, :].astype(jnp.bfloat16)
                    placed = jnp.dot(pick, new, preferred_element_type=jnp.float32)
                    old = buf[r, j, hd].astype(jnp.float32)
                    buf[r, j, hd] = jnp.where(inside, placed, old).astype(jnp.bfloat16)

        @pl.when(lax.rem(first, CP) == cp_rank)
        def _():
            insert(first)

        @pl.when((lax.rem(last, CP) == cp_rank) & (last != first))
        def _():
            insert(last)

        pltpu.make_async_copy(kbuf.at[r], nk_hbm.at[r, :, 0], nksem.at[r]).start()
        pltpu.make_async_copy(vbuf.at[r], nv_hbm.at[r, :, 0], nvsem.at[r]).start()


    def raw_scores(r):
        ctx = ctx_ref[r]
        rows = pl.ds(pl.multiple_of(r * TREE, 8), TREE)
        lane = lax.broadcasted_iota(jnp.int32, (TREE, NBLK * BLK), 1)
        pos = (lane // BLK * CP + cp_rank) * BLK + lane % BLK - ctx
        onehot = (pos == lax.broadcasted_iota(jnp.int32, (TREE, NBLK * BLK), 0)).astype(jnp.bfloat16)
        allowed = jnp.dot(mask_ref[r].astype(jnp.float32).astype(jnp.bfloat16), onehot, preferred_element_type=jnp.float32)
        bias = jnp.where((pos < 0) | (allowed > 0.5), 0.0, MASKED)

        stats = jnp.zeros((TREE, HEAD), jnp.float32)
        stat_lane = lax.broadcasted_iota(jnp.int32, (TREE, HEAD), 1)
        scores = []
        for hd in range(KV):
            query = qkv[hd * GROUP:(hd + 1) * GROUP, rows, :].reshape(GROUP * TREE, HEAD).astype(jnp.bfloat16)
            keys = kbuf[r, :, hd].reshape(NBLK * BLK, HEAD)
            scores.append(lax.dot_general(query, keys, (((1,), (1,)), ((), ())), preferred_element_type=jnp.float32))
        return bias, stats, stat_lane, scores

    def finish(r, bias, stats, stat_lane, scores):
        for hd in range(KV):
            vals = vbuf[r, :, hd].reshape(NBLK * BLK, HEAD)
            score = scores[hd].reshape(GROUP, TREE, NBLK * BLK) * (HEAD ** -0.5 * LOG2E) + bias[None]
            top = jnp.max(score, axis=-1, keepdims=True)
            prob = jnp.exp2(score - top)
            total = jnp.sum(prob, axis=-1, keepdims=True)
            mixed = jnp.dot(prob.reshape(GROUP * TREE, NBLK * BLK).astype(jnp.bfloat16), vals, preferred_element_type=jnp.float32)
            for g in range(GROUP):
                head = hd * GROUP + g
                o_ref[r, :, head * HEAD:(head + 1) * HEAD] = mixed[g * TREE:(g + 1) * TREE]
                stats = jnp.where(stat_lane == head, top[g], stats)
                stats = jnp.where(stat_lane == HEADS + head, total[g], stats)
        o_ref[r, :, WIDE:] = stats


    def attend_step(i, carry):
        group = [i * UNROLL + k for k in range(UNROLL)]
        for r in group:
            prepare(r)
        held = [raw_scores(r) for r in group]
        for r, values in zip(group, held):
            finish(r, *values)
        return carry

    lax.fori_loop(0, EARLY // UNROLL, attend_step, 0)

    def rest(r, carry):
        prepare(r)
        return carry

    lax.fori_loop(EARLY, REQ, rest, 0)

    def drain(r, carry):
        pltpu.make_async_copy(kbuf.at[r], nk_hbm.at[r, :, 0], nksem.at[r]).wait()
        pltpu.make_async_copy(vbuf.at[r], nv_hbm.at[r, :, 0], nvsem.at[r]).wait()
        return carry

    lax.fori_loop(0, REQ, drain, 0)


def merge(a, b):
    ta, tb = a[:, WIDE:], b[:, WIDE:]
    top = jnp.maximum(ta, tb)
    fa, fb = jnp.exp2(ta - top), jnp.exp2(tb - top)
    total = ta * pltpu.roll(fa, HEADS, 1) + tb * pltpu.roll(fb, HEADS, 1)
    lane = lax.broadcasted_iota(jnp.int32, (TREE, HEAD), 1)
    return fa, fb, total, jnp.where(lane < HEADS, top, total)


def main_kernel(ctx_ref, mask_ref, qkv, early, k_hbm, v_hbm, w_hbm, x_hbm, y_ref,
                kbuf, vbuf, late, pin, yrecv, heads, hbf, wbuf, xbuf,
                part, in_end, in_mid, fin, fin_y, fin_c, fin_cy,
                ksem, vsem, wsem, xsem, s_p, r_p, s_y, r_y, s_a, r_a,
                s_e, r_e, s_m, r_m, s_f, r_f, s_yf, r_yf, s_cf, r_cf, s_cy, r_cy):
    cp_rank = lax.axis_index('cp')
    z = lax.axis_index('tp')
    yy = cp_rank // 2
    core = cp_rank % 2
    other_core = 1 - core
    other_y = 1 - yy
    mid = (z + 1) // 2 % 2
    partner = {'cp': yy * 2 + other_core}
    across = {'cp': other_y * 2 + core}
    pair = {'tp': z + 1 - 2 * (z % 2)}
    middle = {'tp': 3 - z}

    def remote(src, dst, send, recv, peer):
        return pltpu.make_async_remote_copy(src_ref=src, dst_ref=dst, send_sem=send, recv_sem=recv, device_id=peer, device_id_type=MESH)

    barrier = pltpu.get_barrier_semaphore()
    for peer in (partner, across, pair):
        pl.semaphore_signal(barrier, inc=1, device_id=peer, device_id_type=MESH)

    @pl.when(mid == 1)
    def _():
        pl.semaphore_signal(barrier, inc=1, device_id=middle, device_id_type=MESH)

    for r in range(EARLY, REQ):
        slot = r - EARLY
        pltpu.make_async_copy(k_hbm.at[r, :, 0], kbuf.at[slot], ksem.at[slot]).start()
        pltpu.make_async_copy(v_hbm.at[r, :, 0], vbuf.at[slot], vsem.at[slot]).start()

    def weight_copy(j):
        cols = pl.ds(pl.multiple_of(core * HALF + j * W, W), W)
        return pltpu.make_async_copy(w_hbm.at[:, cols], wbuf.at[j], wsem.at[j])

    def start_weight(j, carry):
        weight_copy(j).start()
        return carry

    x_copies = [pltpu.make_async_copy(
        x_hbm.at[pl.ds(pl.multiple_of(w * WAVE_ROWS + yy * PART_ROWS, 16), PART_ROWS), pl.ds(pl.multiple_of(core * HALF, HALF), HALF)],
        xbuf.at[w], xsem.at[w]) for w in range(WAVES)]
    def raw_scores(r):
        slot = r - EARLY
        ctx = ctx_ref[r]
        rows = pl.ds(pl.multiple_of(r * TREE, 8), TREE)
        lane = lax.broadcasted_iota(jnp.int32, (TREE, NBLK * BLK), 1)
        pos = (lane // BLK * CP + cp_rank) * BLK + lane % BLK - ctx
        onehot = (pos == lax.broadcasted_iota(jnp.int32, (TREE, NBLK * BLK), 0)).astype(jnp.bfloat16)
        allowed = jnp.dot(mask_ref[r].astype(jnp.float32).astype(jnp.bfloat16), onehot, preferred_element_type=jnp.float32)
        bias = jnp.where((pos < 0) | (allowed > 0.5), 0.0, MASKED)
        scores = []
        for hd in range(KV):
            query = qkv[hd * GROUP:(hd + 1) * GROUP, rows, :].reshape(GROUP * TREE, HEAD).astype(jnp.bfloat16)
            keys = kbuf[slot, :, hd].reshape(NBLK * BLK, HEAD)
            scores.append(lax.dot_general(query, keys, (((1,), (1,)), ((), ())), preferred_element_type=jnp.float32))
        return bias, scores

    def attend(r, bias, scores):
        slot = r - EARLY
        stats = jnp.zeros((TREE, HEAD), jnp.float32)
        stat_lane = lax.broadcasted_iota(jnp.int32, (TREE, HEAD), 1)
        for hd in range(KV):
            vals = vbuf[slot, :, hd].reshape(NBLK * BLK, HEAD)
            score = scores[hd].reshape(GROUP, TREE, NBLK * BLK) * (HEAD ** -0.5 * LOG2E) + bias[None]
            top = jnp.max(score, axis=-1, keepdims=True)
            prob = jnp.exp2(score - top)
            total = jnp.sum(prob, axis=-1, keepdims=True)
            mixed = jnp.dot(prob.reshape(GROUP * TREE, NBLK * BLK).astype(jnp.bfloat16), vals, preferred_element_type=jnp.float32)
            for g in range(GROUP):
                head = hd * GROUP + g
                late[slot, :, head * HEAD:(head + 1) * HEAD] = mixed[g * TREE:(g + 1) * TREE]
                stats = jnp.where(stat_lane == head, top[g], stats)
                stats = jnp.where(stat_lane == HEADS + head, total[g], stats)
        late[slot, :, WIDE:] = stats

    def enter():
        @pl.when(mid == 1)
        def _():
            pl.semaphore_wait(barrier, 4)

        @pl.when(mid == 0)
        def _():
            pl.semaphore_wait(barrier, 3)

    def own(w, chip, to_core):
        return late.at[2 * chip + to_core] if w == WAVES - 1 else early.at[4 * w + 2 * chip + to_core]

    def chip_copy(w, side):
        chip = yy if side else other_y
        return remote(own(w, chip, other_core), pin.at[w, side], s_p.at[w, side], r_p.at[w, side], partner)

    def exchange(w):
        for side in (0, 1):
            chip_copy(w, side).start()

    def y_copy(w):
        return remote(pin.at[w, 0], yrecv.at[w], s_y.at[w], r_y.at[w], across)

    def blend(a, b):
        fa, fb, total, stats = merge(a, b)
        for h in range(HEADS):
            cols = slice(h * HEAD, (h + 1) * HEAD)
            b[:, cols] = a[:, cols] * fa[:, h:h + 1] + b[:, cols] * fb[:, h:h + 1]
        b[:, WIDE:] = stats

    def head_copy(w, owner):
        return remote(heads.at[w, owner], heads.at[w, owner], s_a.at[w], r_a.at[w], partner)

    def finish_start(w):
        y_copy(w).wait_recv()
        a, b, out = pin.at[w, 1], yrecv.at[w], heads.at[w, core]
        fa, fb, total, stats = merge(a, b)
        inv = 1.0 / total
        for h in range(HEADS):
            cols = slice(h * HEAD, (h + 1) * HEAD)
            mixed = a[:, cols] * fa[:, h:h + 1] + b[:, cols] * fb[:, h:h + 1]
            out[:, cols] = mixed * inv[:, HEADS + h:HEADS + h + 1]
        head_copy(w, core).start()

    def finish_end(w):
        head_copy(w, other_core).wait_recv()
        hbf[...] = heads[w].reshape(PART_ROWS, WIDE).astype(jnp.bfloat16)

    def blend_across(w):
        chip_copy(w, 0).wait_recv()
        blend(own(w, other_y, core), pin.at[w, 0])
        y_copy(w).start()

    def blend_mine(w):
        chip_copy(w, 1).wait_recv()
        blend(own(w, yy, core), pin.at[w, 1])

    def pair_step(i, carry):
        pair_of = [EARLY + UNROLL * i + k for k in range(UNROLL)]
        for r in pair_of:
            slot = r - EARLY
            pltpu.make_async_copy(k_hbm.at[r, :, 0], kbuf.at[slot], ksem.at[slot]).wait()
            pltpu.make_async_copy(v_hbm.at[r, :, 0], vbuf.at[slot], vsem.at[slot]).wait()

        @pl.when(i == 0)
        def _():
            lax.fori_loop(0, NP, start_weight, 0)
            for copy in x_copies:
                copy.start()

        held = [raw_scores(r) for r in pair_of]
        for r, values in zip(pair_of, held):
            attend(r, *values)

        @pl.when(i == 0)
        def _():
            blend_across(0)

        @pl.when(i == 1)
        def _():
            exchange(2)
            blend_across(1)
            blend_mine(0)
            blend_mine(1)
        return carry

    enter()
    exchange(0)
    exchange(1)
    lax.fori_loop(0, LATE // UNROLL, pair_step, 0)
    for copy in x_copies:
        copy.wait()
    finish_start(0)
    blend_across(2)
    finish_end(0)

    def end_copy(p):
        return remote(part.at[p], in_end.at[p], s_e, r_e.at[p], pair)

    def mid_copy(p):
        return remote(part.at[p], in_mid.at[p], s_m, r_m.at[p], middle)

    def fin_copy(p):
        return remote(fin.at[p], fin.at[p], s_f, r_f.at[p], pair)

    def across_copy(p):
        return remote(fin.at[p], fin_y.at[p], s_yf, r_yf.at[p], across)

    def core_copy(p):
        return remote(fin.at[p], fin_c.at[p], s_cf, r_cf.at[p], partner)

    def core_y_copy(p):
        return remote(fin_y.at[p], fin_cy.at[p], s_cy, r_cy.at[p], partner)

    def project(p):
        j = p % NP

        @pl.when(p < NP)
        def _():
            weight_copy(j).wait()

        prod = jnp.dot(hbf[...], wbuf[j], preferred_element_type=jnp.float32)
        part[p] = prod.astype(jnp.bfloat16).astype(jnp.float32)

        @pl.when(mid == 0)
        def _():
            end_copy(p).start()

    def emit(buf, p, chip, half):
        rows = pl.ds(pl.multiple_of(p // NP * WAVE_ROWS + chip * PART_ROWS, 16), PART_ROWS)
        cols = pl.ds(pl.multiple_of(half * HALF + p % NP * W, W), W)
        y_ref[rows, cols] = buf[p].astype(jnp.bfloat16)

    def take_end(p):
        end_copy(p).wait_recv()
        part[p] = part[p] + in_end[p]
        mid_copy(p).start()

    def take_mid(p):
        mid_copy(p).wait_recv()
        xcols = pl.ds(pl.multiple_of(p % NP * W, W), W)
        fin[p] = (part[p] + in_mid[p]) + xbuf[p // NP, :, xcols].astype(jnp.float32)
        fin_copy(p).start()
        across_copy(p).start()
        core_copy(p).start()
        emit(fin, p, yy, core)

    def take_fin(p):
        fin_copy(p).wait_recv()
        across_copy(p).start()
        core_copy(p).start()
        emit(fin, p, yy, core)

    def take_core(p):
        core_copy(p).wait_recv()
        emit(fin_c, p, yy, other_core)

    def take_across(p):
        across_copy(p).wait_recv()
        core_y_copy(p).start()
        emit(fin_y, p, other_y, core)

    def take_core_y(p):
        core_y_copy(p).wait_recv()
        emit(fin_cy, p, other_y, other_core)

    def ahead_step(p, carry):
        project(p)
        return carry

    lax.fori_loop(0, AHEAD, ahead_step, 0)
    blend_mine(2)
    lag = lambda at_mid, at_end: jnp.where(mid == 1, at_mid, at_end)
    lag_core, lag_across, lag_core_y = lag(5, 8), lag(7, 10), lag(9, 12)

    def step(s, carry):
        for w in range(1, WAVES):
            @pl.when(s == w * NP - AHEAD - 4)
            def _():
                finish_start(w)

            @pl.when(s == w * NP - AHEAD)
            def _():
                finish_end(w)

        @pl.when(s + AHEAD < PIECES)
        def _():
            project(s + AHEAD)

        @pl.when((mid == 1) & (s < PIECES))
        def _():
            take_end(s)

        @pl.when((mid == 1) & (s >= 3) & (s < PIECES + 3))
        def _():
            take_mid(s - 3)

        @pl.when((mid == 0) & (s >= 6) & (s < PIECES + 6))
        def _():
            take_fin(s - 6)

        for this_lag, body in ((lag_core, take_core), (lag_across, take_across), (lag_core_y, take_core_y)):
            p = s - this_lag

            @pl.when((p >= 0) & (p < PIECES))
            def _():
                body(p)
        return carry

    lax.fori_loop(0, PIECES + 12, step, 0)

    for w in range(WAVES):
        for side in (0, 1):
            chip_copy(w, side).wait_send()
        y_copy(w).wait_send()
        head_copy(w, core).wait_send()

    remote(fin, fin_y, s_yf, r_yf.at[0], across).wait_send()
    remote(fin, fin_c, s_cf, r_cf.at[0], partner).wait_send()
    remote(fin_y, fin_cy, s_cy, r_cy.at[0], partner).wait_send()

    @pl.when(mid == 1)
    def _():
        remote(part, in_mid, s_m, r_m.at[0], middle).wait_send()
        remote(fin, fin, s_f, r_f.at[0], pair).wait_send()

    @pl.when(mid == 0)
    def _():
        remote(part, in_end, s_e, r_e.at[0], pair).wait_send()


def solution(mesh):
    cache_spec = P('dp', None, 'cp', 'tp')
    row_spec = P('dp')
    anywhere = pl.BlockSpec(memory_space=pl.ANY)
    vmem = pl.BlockSpec(memory_space=pltpu.VMEM)
    smem = pl.BlockSpec(memory_space=pltpu.SMEM)
    dma = pltpu.SemaphoreType.DMA
    f32, bf16 = jnp.float32, jnp.bfloat16

    def local_step(hidden, attn_gain, w_query, w_key, w_value, w_out, cache_k, cache_v, ctx_len, positions, tree_mask):
        cos_tab, sin_tab = rope_tables(positions)
        flat = hidden.reshape(ROWS, D)
        cache_shape = jax.ShapeDtypeStruct(cache_k.shape, bf16)
        early_out, heads_qkv, new_k, new_v = pl.pallas_call(
            attend_kernel,
            out_shape=(pltpu.VMEM((EARLY, TREE, EXT), f32), pltpu.VMEM((HEADS + 2 * KV, ROWS, HEAD), f32), cache_shape, cache_shape),
            in_specs=[smem, vmem, vmem, vmem, vmem] + [anywhere] * 6,
            out_specs=(vmem, vmem, anywhere, anywhere),
            scratch_shapes=[
                pltpu.VMEM((ROWS, D), bf16), pltpu.VMEM((ROWS, D), bf16), pltpu.VMEM((2, ROWS, HEAD), f32), pltpu.VMEM((RING, D, TILE), bf16),
                pltpu.VMEM((REQ, NBLK, KV, BLK, HEAD), bf16), pltpu.VMEM((REQ, NBLK, KV, BLK, HEAD), bf16),
                dma((XCHUNKS,)), dma((RING,)), dma((REQ,)), dma((REQ,)), dma((REQ,)), dma((REQ,)),
            ],
            compiler_params=pltpu.CompilerParams(vmem_limit_bytes=54 * 1024 * 1024),
            cost_estimate=pl.CostEstimate(flops=15_000_000_000, bytes_accessed=72_000_000, transcendentals=4_000_000),
            name='attend',
        )(ctx_len, attn_gain, pltpu.with_memory_space_constraint(cos_tab, pltpu.VMEM), pltpu.with_memory_space_constraint(sin_tab, pltpu.VMEM), tree_mask, flat, w_query, w_key, w_value, cache_k, cache_v)
        pieces = pltpu.VMEM((PIECES, PART_ROWS, W), f32)
        out = pl.pallas_call(
            main_kernel,
            out_shape=pltpu.VMEM((ROWS, D), bf16),
            in_specs=[smem, vmem, vmem, vmem] + [anywhere] * 4,
            out_specs=vmem,
            scratch_shapes=[
                pltpu.VMEM((LATE, NBLK, KV, BLK, HEAD), bf16), pltpu.VMEM((LATE, NBLK, KV, BLK, HEAD), bf16),
                pltpu.VMEM((LATE, TREE, EXT), f32), pltpu.VMEM((WAVES, 2, TREE, EXT), f32), pltpu.VMEM((WAVES, TREE, EXT), f32), pltpu.VMEM((WAVES, 2, TREE, WIDE), f32),
                pltpu.VMEM((PART_ROWS, WIDE), bf16), pltpu.VMEM((NP, WIDE, W), bf16), pltpu.VMEM((WAVES, PART_ROWS, HALF), bf16),
                pieces, pieces, pieces, pieces, pieces, pieces, pieces,
                dma((LATE,)), dma((LATE,)), dma((NP,)), dma((WAVES,)), dma((WAVES, 2)), dma((WAVES, 2)), dma((WAVES,)), dma((WAVES,)), dma((WAVES,)), dma((WAVES,)),
            ] + [dma, dma((PIECES,))] * 6,
            compiler_params=pltpu.CompilerParams(vmem_limit_bytes=50 * 1024 * 1024, collective_id=0, has_side_effects=True),
            cost_estimate=pl.CostEstimate(flops=5_000_000_000, bytes_accessed=42_000_000, transcendentals=5_000_000),
            name='main',
        )(ctx_len, tree_mask, pltpu.with_memory_space_constraint(heads_qkv, pltpu.VMEM), pltpu.with_memory_space_constraint(early_out, pltpu.VMEM), new_k, new_v, w_out, flat)
        return out.reshape(REQ, TREE, D), new_k, new_v

    return jax.shard_map(local_step, mesh=mesh, in_specs=(row_spec, P(), P(None, 'tp'), P(None, 'tp'), P(None, 'tp'), P('tp', None), cache_spec, cache_spec, row_spec, row_spec, row_spec), out_specs=(row_spec, cache_spec, cache_spec), check_vma=False)
```

```python
import math
import jax
import jax.numpy as jnp
from jax import lax
from jax.experimental import pallas as pl
from jax.experimental.pallas import tpu as pltpu
from jax.sharding import PartitionSpec as P

ROPE_THETA = 500000.0
NORM_EPS = 1e-5
MASKED = -1e30
UNROLL = 2
LOG2E = 1.4426950408889634
MESH = pl.DeviceIdType.MESH

REQ = 12
TREE = 24
ROWS = REQ * TREE
D = 8192
HEAD = 128
KV = 2
GROUP = 8
HEADS = KV * GROUP
NBLK = 4
BLK = 256
CP = 4
WIDE = HEADS * HEAD
EXT = WIDE + HEAD
TILE = 256
NTILE = (HEADS + 2 * KV) * HEAD // TILE // 2
XCHUNKS = 3
STEPS_AHEAD = 2
EARLY = 8
LATE = REQ - EARLY
HALF = D // 2
NP = 16
W = HALF // NP
WAVES = 3
WAVE_ROWS = CP * TREE
PART_ROWS = WAVE_ROWS // 2
PIECES = WAVES * NP
AHEAD = 8


def rope_tables(positions):
    freq_idx = jnp.arange(HEAD // 2, dtype=jnp.float32)
    inv_freq = 1.0 / (ROPE_THETA ** (2.0 * freq_idx / HEAD))
    wavelen = 2.0 * math.pi / inv_freq
    smooth = (8192.0 / wavelen - 1.0) / 3.0
    blended = (1.0 - smooth) * inv_freq / 8.0 + smooth * inv_freq
    inv_freq = jnp.where(wavelen < 2048.0, inv_freq, jnp.where(wavelen > 8192.0, inv_freq / 8.0, blended))
    angle = positions.astype(jnp.float32)[..., None] * inv_freq
    return jnp.cos(angle).reshape(ROWS, HEAD // 2), jnp.sin(angle).reshape(ROWS, HEAD // 2)


def project_kernel(cos_ref, sin_ref, gain_hbm, x_hbm, wq_hbm, wk_hbm, wv_hbm, qkv,
                   x_ref, gain_ref, h_ref, turn, wbuf, xsem, gsem, wsem, s_q, r_q):
    cp_rank = lax.axis_index('cp')
    core = cp_rank % 2
    partner = {'cp': cp_rank + 1 - 2 * core}

    x_copies = []
    for k in range(XCHUNKS):
        rows = pl.ds(k * (ROWS // XCHUNKS), ROWS // XCHUNKS)
        x_copies.append(pltpu.make_async_copy(x_hbm.at[rows, :], x_ref.at[rows, :], xsem.at[k]))
        x_copies[k].start()
    gain_copy = pltpu.make_async_copy(gain_hbm, gain_ref, gsem)
    gain_copy.start()
    barrier = pltpu.get_barrier_semaphore()
    pl.semaphore_signal(barrier, inc=1, device_id=partner, device_id_type=MESH)

    def start_weights():
        one = pl.ds(pl.multiple_of(core * HEAD, HEAD), HEAD)
        pltpu.make_async_copy(wk_hbm.at[:, one], wbuf.at[0, :, :HEAD], wsem.at[0]).start()
        pltpu.make_async_copy(wv_hbm.at[:, one], wbuf.at[0, :, HEAD:], wsem.at[0]).start()
        for i in range(1, NTILE):
            cols = pl.ds(pl.multiple_of(core * (WIDE // 2) + (i - 1) * TILE, TILE), TILE)
            pltpu.make_async_copy(wq_hbm.at[:, cols], wbuf.at[i], wsem.at[i]).start()

    turn[0] = jnp.concatenate([cos_ref[...], cos_ref[...]], axis=-1)
    turn[1] = jnp.concatenate([-sin_ref[...], sin_ref[...]], axis=-1)
    def norm_step(i, carry):
        rows = pl.ds(pl.multiple_of(i * 16, 16), 16)
        squares = [jnp.zeros((16, HEAD), jnp.float32) for _ in range(2)]
        for k in range(D // HEAD):
            wide = x_ref[rows, k * HEAD:(k + 1) * HEAD].astype(jnp.float32)
            squares[k % 2] = squares[k % 2] + wide * wide
        inv = lax.rsqrt(jnp.sum(squares[0] + squares[1], axis=-1, keepdims=True) * (1.0 / D) + NORM_EPS)
        for k in range(D // HEAD):
            cols = slice(k * HEAD, (k + 1) * HEAD)
            wide = x_ref[rows, cols].astype(jnp.float32)
            h_ref[rows, cols] = (wide * inv * gain_ref[cols].astype(jnp.float32).reshape(1, HEAD)).astype(jnp.bfloat16)
        return carry

    gain_copy.wait()
    for k in range(XCHUNKS):
        x_copies[k].wait()
        if k == 0:
            start_weights()
        lax.fori_loop(k * (ROWS // 16 // XCHUNKS), (k + 1) * (ROWS // 16 // XCHUNKS), norm_step, 0)
    pl.semaphore_wait(barrier, 1)

    def head_copy(head, n):
        return pltpu.make_async_remote_copy(src_ref=qkv.at[head], dst_ref=qkv.at[head], send_sem=s_q, recv_sem=r_q.at[n], device_id=partner, device_id_type=MESH)

    def proj_step(i, carry):
        pltpu.make_async_copy(wq_hbm.at[:, :TILE], wbuf.at[i], wsem.at[i]).wait()
        acc = jnp.dot(h_ref[...], wbuf[i], preferred_element_type=jnp.float32)
        for hh in range(2):
            part = acc[:, hh * HEAD:(hh + 1) * HEAD]
            turned = pltpu.roll(part, HEAD // 2, 1)
            cos_tab, sin_tab = turn[0], turn[1]
            if hh == 1:
                cos_tab = jnp.where(i > 0, cos_tab, 1.0)
                sin_tab = jnp.where(i > 0, sin_tab, 0.0)
            head = jnp.where(i == 0, HEADS + KV * hh + core, GROUP * core + 2 * (i - 1) + hh)
            qkv[head] = part * cos_tab + turned * sin_tab
            head_copy(head, 2 * i + hh).start()
        return carry

    lax.fori_loop(0, NTILE, proj_step, 0)
    for n in range(2 * NTILE):
        head_copy(0, n).wait_recv()
    half = qkv.at[pl.ds(0, 2 * NTILE)]
    pltpu.make_async_remote_copy(src_ref=half, dst_ref=half, send_sem=s_q, recv_sem=r_q.at[0], device_id=partner, device_id_type=MESH).wait_send()


def attend_kernel(ctx_ref, mask_ref, qkv, ck_hbm, cv_hbm,
                  o_ref, nk_hbm, nv_hbm,
                  kbuf, vbuf, ksem, vsem, nksem, nvsem):
    cp_rank = lax.axis_index('cp')

    def start_cache(r):
        pltpu.make_async_copy(ck_hbm.at[r, :, 0], kbuf.at[r], ksem.at[r]).start()
        pltpu.make_async_copy(cv_hbm.at[r, :, 0], vbuf.at[r], vsem.at[r]).start()

    def start_step(i):
        for k in range(UNROLL):
            start_cache(UNROLL * i + k)
        start_cache(EARLY + i)

    for i in range(STEPS_AHEAD):
        start_step(i)

    def prepare(r):
        pltpu.make_async_copy(ck_hbm.at[r, :, 0], kbuf.at[r], ksem.at[r]).wait()
        pltpu.make_async_copy(cv_hbm.at[r, :, 0], vbuf.at[r], vsem.at[r]).wait()
        ctx = ctx_ref[r]
        rows = pl.ds(pl.multiple_of(r * TREE, 8), TREE)
        first = ctx // BLK
        last = (ctx + TREE - 1) // BLK

        def insert(block):
            j = block // CP
            slot_of = lax.broadcasted_iota(jnp.int32, (BLK, TREE), 0) + (block * BLK - ctx)
            pick = (slot_of == lax.broadcasted_iota(jnp.int32, (BLK, TREE), 1)).astype(jnp.bfloat16)
            wide_slot = lax.broadcasted_iota(jnp.int32, (BLK, HEAD), 0) + (block * BLK - ctx)
            inside = (wide_slot >= 0) & (wide_slot < TREE)
            for hd in range(KV):
                for buf, base in ((kbuf, HEADS), (vbuf, HEADS + KV)):
                    new = qkv[base + hd, rows, :].astype(jnp.bfloat16)
                    placed = jnp.dot(pick, new, preferred_element_type=jnp.float32)
                    old = buf[r, j, hd].astype(jnp.float32)
                    buf[r, j, hd] = jnp.where(inside, placed, old).astype(jnp.bfloat16)

        @pl.when(lax.rem(first, CP) == cp_rank)
        def _():
            insert(first)

        @pl.when((lax.rem(last, CP) == cp_rank) & (last != first))
        def _():
            insert(last)

        pltpu.make_async_copy(kbuf.at[r], nk_hbm.at[r, :, 0], nksem.at[r]).start()
        pltpu.make_async_copy(vbuf.at[r], nv_hbm.at[r, :, 0], nvsem.at[r]).start()


    def raw_scores(r):
        ctx = ctx_ref[r]
        rows = pl.ds(pl.multiple_of(r * TREE, 8), TREE)
        lane = lax.broadcasted_iota(jnp.int32, (TREE, NBLK * BLK), 1)
        pos = (lane // BLK * CP + cp_rank) * BLK + lane % BLK - ctx
        onehot = (pos == lax.broadcasted_iota(jnp.int32, (TREE, NBLK * BLK), 0)).astype(jnp.bfloat16)
        allowed = jnp.dot(mask_ref[r].astype(jnp.float32).astype(jnp.bfloat16), onehot, preferred_element_type=jnp.float32)
        bias = jnp.where((pos < 0) | (allowed > 0.5), 0.0, MASKED)

        stats = jnp.zeros((TREE, HEAD), jnp.float32)
        stat_lane = lax.broadcasted_iota(jnp.int32, (TREE, HEAD), 1)
        scores = []
        for hd in range(KV):
            query = qkv[hd * GROUP:(hd + 1) * GROUP, rows, :].reshape(GROUP * TREE, HEAD).astype(jnp.bfloat16)
            keys = kbuf[r, :, hd].reshape(NBLK * BLK, HEAD)
            scores.append(lax.dot_general(query, keys, (((1,), (1,)), ((), ())), preferred_element_type=jnp.float32))
        return bias, stats, stat_lane, scores

    def finish(r, bias, stats, stat_lane, scores):
        for hd in range(KV):
            vals = vbuf[r, :, hd].reshape(NBLK * BLK, HEAD)
            score = scores[hd].reshape(GROUP, TREE, NBLK * BLK) * (HEAD ** -0.5 * LOG2E) + bias[None]
            top = jnp.max(score, axis=-1, keepdims=True)
            prob = jnp.exp2(score - top)
            total = jnp.sum(prob, axis=-1, keepdims=True)
            mixed = jnp.dot(prob.reshape(GROUP * TREE, NBLK * BLK).astype(jnp.bfloat16), vals, preferred_element_type=jnp.float32)
            for g in range(GROUP):
                head = hd * GROUP + g
                o_ref[r, :, head * HEAD:(head + 1) * HEAD] = mixed[g * TREE:(g + 1) * TREE]
                stats = jnp.where(stat_lane == head, top[g], stats)
                stats = jnp.where(stat_lane == HEADS + head, total[g], stats)
        o_ref[r, :, WIDE:] = stats


    def attend_step(i, carry):
        @pl.when(i + STEPS_AHEAD < EARLY // UNROLL)
        def _():
            start_step(i + STEPS_AHEAD)

        group = [i * UNROLL + k for k in range(UNROLL)]
        for r in group:
            prepare(r)
        held = [raw_scores(r) for r in group]
        for r, values in zip(group, held):
            finish(r, *values)
        prepare(EARLY + i)
        return carry

    lax.fori_loop(0, EARLY // UNROLL, attend_step, 0)

    def drain(r, carry):
        pltpu.make_async_copy(kbuf.at[r], nk_hbm.at[r, :, 0], nksem.at[r]).wait()
        pltpu.make_async_copy(vbuf.at[r], nv_hbm.at[r, :, 0], nvsem.at[r]).wait()
        return carry

    lax.fori_loop(0, REQ, drain, 0)


def merge(a, b):
    ta, tb = a[:, WIDE:], b[:, WIDE:]
    top = jnp.maximum(ta, tb)
    fa, fb = jnp.exp2(ta - top), jnp.exp2(tb - top)
    total = ta * pltpu.roll(fa, HEADS, 1) + tb * pltpu.roll(fb, HEADS, 1)
    lane = lax.broadcasted_iota(jnp.int32, (TREE, HEAD), 1)
    return fa, fb, total, jnp.where(lane < HEADS, top, total)


def main_kernel(ctx_ref, mask_ref, qkv, early, k_hbm, v_hbm, w_hbm, x_hbm, y_ref,
                kbuf, vbuf, late, pin, yrecv, heads, hbf, wbuf, xbuf,
                part, in_end, in_mid, fin, fin_y, fin_c, fin_cy,
                ksem, vsem, wsem, xsem, s_p, r_p, s_y, r_y, s_a, r_a,
                s_e, r_e, s_m, r_m, s_f, r_f, s_yf, r_yf, s_cf, r_cf, s_cy, r_cy):
    cp_rank = lax.axis_index('cp')
    z = lax.axis_index('tp')
    yy = cp_rank // 2
    core = cp_rank % 2
    other_core = 1 - core
    other_y = 1 - yy
    mid = (z + 1) // 2 % 2
    partner = {'cp': yy * 2 + other_core}
    across = {'cp': other_y * 2 + core}
    pair = {'tp': z + 1 - 2 * (z % 2)}
    middle = {'tp': 3 - z}

    def remote(src, dst, send, recv, peer):
        return pltpu.make_async_remote_copy(src_ref=src, dst_ref=dst, send_sem=send, recv_sem=recv, device_id=peer, device_id_type=MESH)

    barrier = pltpu.get_barrier_semaphore()
    for peer in (partner, across, pair):
        pl.semaphore_signal(barrier, inc=1, device_id=peer, device_id_type=MESH)

    @pl.when(mid == 1)
    def _():
        pl.semaphore_signal(barrier, inc=1, device_id=middle, device_id_type=MESH)

    for r in range(EARLY, REQ):
        slot = r - EARLY
        pltpu.make_async_copy(k_hbm.at[r, :, 0], kbuf.at[slot], ksem.at[slot]).start()
        pltpu.make_async_copy(v_hbm.at[r, :, 0], vbuf.at[slot], vsem.at[slot]).start()

    def weight_copy(j):
        cols = pl.ds(pl.multiple_of(core * HALF + j * W, W), W)
        return pltpu.make_async_copy(w_hbm.at[:, cols], wbuf.at[j], wsem.at[j])

    def start_weight(j, carry):
        weight_copy(j).start()
        return carry

    x_copies = [pltpu.make_async_copy(
        x_hbm.at[pl.ds(pl.multiple_of(w * WAVE_ROWS + yy * PART_ROWS, 16), PART_ROWS), pl.ds(pl.multiple_of(core * HALF, HALF), HALF)],
        xbuf.at[w], xsem.at[w]) for w in range(WAVES)]
    def raw_scores(r):
        slot = r - EARLY
        ctx = ctx_ref[r]
        rows = pl.ds(pl.multiple_of(r * TREE, 8), TREE)
        lane = lax.broadcasted_iota(jnp.int32, (TREE, NBLK * BLK), 1)
        pos = (lane // BLK * CP + cp_rank) * BLK + lane % BLK - ctx
        onehot = (pos == lax.broadcasted_iota(jnp.int32, (TREE, NBLK * BLK), 0)).astype(jnp.bfloat16)
        allowed = jnp.dot(mask_ref[r].astype(jnp.float32).astype(jnp.bfloat16), onehot, preferred_element_type=jnp.float32)
        bias = jnp.where((pos < 0) | (allowed > 0.5), 0.0, MASKED)
        scores = []
        for hd in range(KV):
            query = qkv[hd * GROUP:(hd + 1) * GROUP, rows, :].reshape(GROUP * TREE, HEAD).astype(jnp.bfloat16)
            keys = kbuf[slot, :, hd].reshape(NBLK * BLK, HEAD)
            scores.append(lax.dot_general(query, keys, (((1,), (1,)), ((), ())), preferred_element_type=jnp.float32))
        return bias, scores

    def attend(r, bias, scores):
        slot = r - EARLY
        stats = jnp.zeros((TREE, HEAD), jnp.float32)
        stat_lane = lax.broadcasted_iota(jnp.int32, (TREE, HEAD), 1)
        for hd in range(KV):
            vals = vbuf[slot, :, hd].reshape(NBLK * BLK, HEAD)
            score = scores[hd].reshape(GROUP, TREE, NBLK * BLK) * (HEAD ** -0.5 * LOG2E) + bias[None]
            top = jnp.max(score, axis=-1, keepdims=True)
            prob = jnp.exp2(score - top)
            total = jnp.sum(prob, axis=-1, keepdims=True)
            mixed = jnp.dot(prob.reshape(GROUP * TREE, NBLK * BLK).astype(jnp.bfloat16), vals, preferred_element_type=jnp.float32)
            for g in range(GROUP):
                head = hd * GROUP + g
                late[slot, :, head * HEAD:(head + 1) * HEAD] = mixed[g * TREE:(g + 1) * TREE]
                stats = jnp.where(stat_lane == head, top[g], stats)
                stats = jnp.where(stat_lane == HEADS + head, total[g], stats)
        late[slot, :, WIDE:] = stats

    def enter():
        @pl.when(mid == 1)
        def _():
            pl.semaphore_wait(barrier, 4)

        @pl.when(mid == 0)
        def _():
            pl.semaphore_wait(barrier, 3)

    def own(w, chip, to_core):
        return late.at[2 * chip + to_core] if w == WAVES - 1 else early.at[4 * w + 2 * chip + to_core]

    def chip_copy(w, side):
        chip = yy if side else other_y
        return remote(own(w, chip, other_core), pin.at[w, side], s_p.at[w, side], r_p.at[w, side], partner)

    def exchange(w):
        for side in (0, 1):
            chip_copy(w, side).start()

    def y_copy(w):
        return remote(pin.at[w, 0], yrecv.at[w], s_y.at[w], r_y.at[w], across)

    def blend(a, b):
        fa, fb, total, stats = merge(a, b)
        for h in range(HEADS):
            cols = slice(h * HEAD, (h + 1) * HEAD)
            b[:, cols] = a[:, cols] * fa[:, h:h + 1] + b[:, cols] * fb[:, h:h + 1]
        b[:, WIDE:] = stats

    def head_copy(w, owner):
        return remote(heads.at[w, owner], heads.at[w, owner], s_a.at[w], r_a.at[w], partner)

    def finish_start(w):
        y_copy(w).wait_recv()
        a, b, out = pin.at[w, 1], yrecv.at[w], heads.at[w, core]
        fa, fb, total, stats = merge(a, b)
        inv = 1.0 / total
        for h in range(HEADS):
            cols = slice(h * HEAD, (h + 1) * HEAD)
            mixed = a[:, cols] * fa[:, h:h + 1] + b[:, cols] * fb[:, h:h + 1]
            out[:, cols] = mixed * inv[:, HEADS + h:HEADS + h + 1]
        head_copy(w, core).start()

    def finish_end(w):
        head_copy(w, other_core).wait_recv()
        hbf[...] = heads[w].reshape(PART_ROWS, WIDE).astype(jnp.bfloat16)

    def blend_across(w):
        chip_copy(w, 0).wait_recv()
        blend(own(w, other_y, core), pin.at[w, 0])
        y_copy(w).start()

    def blend_mine(w):
        chip_copy(w, 1).wait_recv()
        blend(own(w, yy, core), pin.at[w, 1])

    def pair_step(i, carry):
        pair_of = [EARLY + UNROLL * i + k for k in range(UNROLL)]
        for r in pair_of:
            slot = r - EARLY
            pltpu.make_async_copy(k_hbm.at[r, :, 0], kbuf.at[slot], ksem.at[slot]).wait()
            pltpu.make_async_copy(v_hbm.at[r, :, 0], vbuf.at[slot], vsem.at[slot]).wait()

        @pl.when(i == 0)
        def _():
            lax.fori_loop(0, NP, start_weight, 0)
            for copy in x_copies:
                copy.start()

        held = [raw_scores(r) for r in pair_of]
        for r, values in zip(pair_of, held):
            attend(r, *values)

        @pl.when(i == 0)
        def _():
            blend_across(0)

        @pl.when(i == 1)
        def _():
            exchange(2)
            blend_across(1)
            blend_mine(0)
            blend_mine(1)
        return carry

    enter()
    exchange(0)
    exchange(1)
    lax.fori_loop(0, LATE // UNROLL, pair_step, 0)
    for copy in x_copies:
        copy.wait()
    finish_start(0)
    blend_across(2)
    finish_end(0)

    def end_copy(p):
        return remote(part.at[p], in_end.at[p], s_e, r_e.at[p], pair)

    def mid_copy(p):
        return remote(part.at[p], in_mid.at[p], s_m, r_m.at[p], middle)

    def fin_copy(p):
        return remote(fin.at[p], fin.at[p], s_f, r_f.at[p], pair)

    def across_copy(p):
        return remote(fin.at[p], fin_y.at[p], s_yf, r_yf.at[p], across)

    def core_copy(p):
        return remote(fin.at[p], fin_c.at[p], s_cf, r_cf.at[p], partner)

    def core_y_copy(p):
        return remote(fin_y.at[p], fin_cy.at[p], s_cy, r_cy.at[p], partner)

    def project(p):
        j = p % NP

        @pl.when(p < NP)
        def _():
            weight_copy(j).wait()

        prod = jnp.dot(hbf[...], wbuf[j], preferred_element_type=jnp.float32)
        part[p] = prod.astype(jnp.bfloat16).astype(jnp.float32)

        @pl.when(mid == 0)
        def _():
            end_copy(p).start()

    def emit(buf, p, chip, half):
        rows = pl.ds(pl.multiple_of(p // NP * WAVE_ROWS + chip * PART_ROWS, 16), PART_ROWS)
        cols = pl.ds(pl.multiple_of(half * HALF + p % NP * W, W), W)
        y_ref[rows, cols] = buf[p].astype(jnp.bfloat16)

    def take_end(p):
        end_copy(p).wait_recv()
        part[p] = part[p] + in_end[p]
        mid_copy(p).start()

    def take_mid(p):
        mid_copy(p).wait_recv()
        xcols = pl.ds(pl.multiple_of(p % NP * W, W), W)
        fin[p] = (part[p] + in_mid[p]) + xbuf[p // NP, :, xcols].astype(jnp.float32)
        fin_copy(p).start()
        across_copy(p).start()
        core_copy(p).start()
        emit(fin, p, yy, core)

    def take_fin(p):
        fin_copy(p).wait_recv()
        across_copy(p).start()
        core_copy(p).start()
        emit(fin, p, yy, core)

    def take_core(p):
        core_copy(p).wait_recv()
        emit(fin_c, p, yy, other_core)

    def take_across(p):
        across_copy(p).wait_recv()
        core_y_copy(p).start()
        emit(fin_y, p, other_y, core)

    def take_core_y(p):
        core_y_copy(p).wait_recv()
        emit(fin_cy, p, other_y, other_core)

    def ahead_step(p, carry):
        project(p)
        return carry

    lax.fori_loop(0, AHEAD, ahead_step, 0)
    blend_mine(2)
    lag = lambda at_mid, at_end: jnp.where(mid == 1, at_mid, at_end)
    lag_core, lag_across, lag_core_y = lag(6, 9), lag(8, 11), lag(10, 13)

    def step(s, carry):
        for w in range(1, WAVES):
            @pl.when(s == w * NP - AHEAD - 4)
            def _():
                finish_start(w)

            @pl.when(s == w * NP - AHEAD)
            def _():
                finish_end(w)

        @pl.when(s + AHEAD < PIECES)
        def _():
            project(s + AHEAD)

        @pl.when((mid == 1) & (s < PIECES))
        def _():
            take_end(s)

        @pl.when((mid == 1) & (s >= 3) & (s < PIECES + 3))
        def _():
            take_mid(s - 3)

        @pl.when((mid == 0) & (s >= 7) & (s < PIECES + 7))
        def _():
            take_fin(s - 7)

        for this_lag, body in ((lag_core, take_core), (lag_across, take_across), (lag_core_y, take_core_y)):
            p = s - this_lag

            @pl.when((p >= 0) & (p < PIECES))
            def _():
                body(p)
        return carry

    lax.fori_loop(0, PIECES + 13, step, 0)

    for w in range(WAVES):
        for side in (0, 1):
            chip_copy(w, side).wait_send()
        y_copy(w).wait_send()
        head_copy(w, core).wait_send()

    remote(fin, fin_y, s_yf, r_yf.at[0], across).wait_send()
    remote(fin, fin_c, s_cf, r_cf.at[0], partner).wait_send()
    remote(fin_y, fin_cy, s_cy, r_cy.at[0], partner).wait_send()

    @pl.when(mid == 1)
    def _():
        remote(part, in_mid, s_m, r_m.at[0], middle).wait_send()
        remote(fin, fin, s_f, r_f.at[0], pair).wait_send()

    @pl.when(mid == 0)
    def _():
        remote(part, in_end, s_e, r_e.at[0], pair).wait_send()


def solution(mesh):
    cache_spec = P('dp', None, 'cp', 'tp')
    row_spec = P('dp')
    anywhere = pl.BlockSpec(memory_space=pl.ANY)
    vmem = pl.BlockSpec(memory_space=pltpu.VMEM)
    smem = pl.BlockSpec(memory_space=pltpu.SMEM)
    dma = pltpu.SemaphoreType.DMA
    f32, bf16 = jnp.float32, jnp.bfloat16

    def local_step(hidden, attn_gain, w_query, w_key, w_value, w_out, cache_k, cache_v, ctx_len, positions, tree_mask):
        cos_tab, sin_tab = rope_tables(positions)
        flat = hidden.reshape(ROWS, D)
        cache_shape = jax.ShapeDtypeStruct(cache_k.shape, bf16)
        heads_qkv = pl.pallas_call(
            project_kernel,
            out_shape=pltpu.VMEM((HEADS + 2 * KV, ROWS, HEAD), f32),
            in_specs=[vmem, vmem, pl.BlockSpec(memory_space=pltpu.HBM)] + [anywhere] * 4,
            out_specs=vmem,
            scratch_shapes=[
                pltpu.VMEM((ROWS, D), bf16), pltpu.VMEM((D,), bf16), pltpu.VMEM((ROWS, D), bf16), pltpu.VMEM((2, ROWS, HEAD), f32), pltpu.VMEM((NTILE, D, TILE), bf16),
                dma((XCHUNKS,)), dma, dma((NTILE,)), dma, dma((2 * NTILE,)),
            ],
            compiler_params=pltpu.CompilerParams(vmem_limit_bytes=50 * 1024 * 1024, collective_id=1, has_side_effects=True),
            cost_estimate=pl.CostEstimate(flops=6_000_000_000, bytes_accessed=26_000_000, transcendentals=1_000),
            name='project',
        )(pltpu.with_memory_space_constraint(cos_tab, pltpu.VMEM), pltpu.with_memory_space_constraint(sin_tab, pltpu.VMEM), pltpu.with_memory_space_constraint(attn_gain, pltpu.HBM), flat, w_query, w_key, w_value)
        heads_qkv = pltpu.with_memory_space_constraint(heads_qkv, pltpu.VMEM)
        early_out, new_k, new_v = pl.pallas_call(
            attend_kernel,
            out_shape=(pltpu.VMEM((EARLY, TREE, EXT), f32), cache_shape, cache_shape),
            in_specs=[smem, vmem, vmem] + [anywhere] * 2,
            out_specs=(vmem, anywhere, anywhere),
            scratch_shapes=[
                pltpu.VMEM((REQ, NBLK, KV, BLK, HEAD), bf16), pltpu.VMEM((REQ, NBLK, KV, BLK, HEAD), bf16),
                dma((REQ,)), dma((REQ,)), dma((REQ,)), dma((REQ,)),
            ],
            compiler_params=pltpu.CompilerParams(vmem_limit_bytes=40 * 1024 * 1024),
            cost_estimate=pl.CostEstimate(flops=3_000_000_000, bytes_accessed=26_000_000, transcendentals=4_000_000),
            name='attend',
        )(ctx_len, tree_mask, heads_qkv, cache_k, cache_v)
        pieces = pltpu.VMEM((PIECES, PART_ROWS, W), f32)
        out = pl.pallas_call(
            main_kernel,
            out_shape=pltpu.VMEM((ROWS, D), bf16),
            in_specs=[smem, vmem, vmem, vmem] + [anywhere] * 4,
            out_specs=vmem,
            scratch_shapes=[
                pltpu.VMEM((LATE, NBLK, KV, BLK, HEAD), bf16), pltpu.VMEM((LATE, NBLK, KV, BLK, HEAD), bf16),
                pltpu.VMEM((LATE, TREE, EXT), f32), pltpu.VMEM((WAVES, 2, TREE, EXT), f32), pltpu.VMEM((WAVES, TREE, EXT), f32), pltpu.VMEM((WAVES, 2, TREE, WIDE), f32),
                pltpu.VMEM((PART_ROWS, WIDE), bf16), pltpu.VMEM((NP, WIDE, W), bf16), pltpu.VMEM((WAVES, PART_ROWS, HALF), bf16),
                pieces, pieces, pieces, pieces, pieces, pieces, pieces,
                dma((LATE,)), dma((LATE,)), dma((NP,)), dma((WAVES,)), dma((WAVES, 2)), dma((WAVES, 2)), dma((WAVES,)), dma((WAVES,)), dma((WAVES,)), dma((WAVES,)),
            ] + [dma, dma((PIECES,))] * 6,
            compiler_params=pltpu.CompilerParams(vmem_limit_bytes=50 * 1024 * 1024, collective_id=0, has_side_effects=True),
            cost_estimate=pl.CostEstimate(flops=5_000_000_000, bytes_accessed=42_000_000, transcendentals=5_000_000),
            name='main',
        )(ctx_len, tree_mask, heads_qkv, pltpu.with_memory_space_constraint(early_out, pltpu.VMEM), new_k, new_v, w_out, flat)
        return out.reshape(REQ, TREE, D), new_k, new_v

    return jax.shard_map(local_step, mesh=mesh, in_specs=(row_spec, P(), P(None, 'tp'), P(None, 'tp'), P(None, 'tp'), P('tp', None), cache_spec, cache_spec, row_spec, row_spec, row_spec), out_specs=(row_spec, cache_spec, cache_spec), check_vma=False)
```

```python
import math
import jax
import jax.numpy as jnp
from jax import lax
from jax.experimental import pallas as pl
from jax.experimental.pallas import tpu as pltpu
from jax.sharding import PartitionSpec as P

ROPE_THETA = 500000.0
NORM_EPS = 1e-5
MASKED = -1e30
UNROLL = 2
LOG2E = 1.4426950408889634
MESH = pl.DeviceIdType.MESH

REQ = 12
TREE = 24
ROWS = REQ * TREE
D = 8192
HEAD = 128
KV = 2
GROUP = 8
HEADS = KV * GROUP
NBLK = 4
BLK = 256
CP = 4
WIDE = HEADS * HEAD
EXT = WIDE + HEAD
TILE = 256
NTILE = (HEADS + 2 * KV) * HEAD // TILE // 2
XCHUNKS = 3
STEPS_AHEAD = 2
EARLY = 8
LATE = REQ - EARLY
HALF = D // 2
NP = 16
W = HALF // NP
WAVES = 3
WAVE_ROWS = CP * TREE
PART_ROWS = WAVE_ROWS // 2
PIECES = WAVES * NP
AHEAD = 8


def rope_tables(positions):
    freq_idx = jnp.arange(HEAD // 2, dtype=jnp.float32)
    inv_freq = 1.0 / (ROPE_THETA ** (2.0 * freq_idx / HEAD))
    wavelen = 2.0 * math.pi / inv_freq
    smooth = (8192.0 / wavelen - 1.0) / 3.0
    blended = (1.0 - smooth) * inv_freq / 8.0 + smooth * inv_freq
    inv_freq = jnp.where(wavelen < 2048.0, inv_freq, jnp.where(wavelen > 8192.0, inv_freq / 8.0, blended))
    angle = positions.astype(jnp.float32)[..., None] * inv_freq
    return jnp.cos(angle).reshape(ROWS, HEAD // 2), jnp.sin(angle).reshape(ROWS, HEAD // 2)


def project_kernel(cos_ref, sin_ref, gain_hbm, x_hbm, wq_hbm, wk_hbm, wv_hbm, qkv,
                   x_ref, gain_ref, h_ref, turn, wbuf, xsem, gsem, wsem, s_q, r_q):
    cp_rank = lax.axis_index('cp')
    core = cp_rank % 2
    partner = {'cp': cp_rank + 1 - 2 * core}

    gain_copy = pltpu.make_async_copy(gain_hbm, gain_ref, gsem)
    gain_copy.start()
    x_copies = []
    for k in range(XCHUNKS):
        rows = pl.ds(k * (ROWS // XCHUNKS), ROWS // XCHUNKS)
        x_copies.append(pltpu.make_async_copy(x_hbm.at[rows, :], x_ref.at[rows, :], xsem.at[k]))
        x_copies[k].start()
    barrier = pltpu.get_barrier_semaphore()
    pl.semaphore_signal(barrier, inc=1, device_id=partner, device_id_type=MESH)

    def start_weights():
        one = pl.ds(pl.multiple_of(core * HEAD, HEAD), HEAD)
        pltpu.make_async_copy(wk_hbm.at[:, one], wbuf.at[0, :, :HEAD], wsem.at[0]).start()
        pltpu.make_async_copy(wv_hbm.at[:, one], wbuf.at[0, :, HEAD:], wsem.at[0]).start()
        for i in range(1, NTILE):
            cols = pl.ds(pl.multiple_of(core * (WIDE // 2) + (i - 1) * TILE, TILE), TILE)
            pltpu.make_async_copy(wq_hbm.at[:, cols], wbuf.at[i], wsem.at[i]).start()

    turn[0] = jnp.concatenate([cos_ref[...], cos_ref[...]], axis=-1)
    turn[1] = jnp.concatenate([-sin_ref[...], sin_ref[...]], axis=-1)
    def norm_step(i, carry):
        rows = pl.ds(pl.multiple_of(i * 16, 16), 16)
        squares = [jnp.zeros((16, HEAD), jnp.float32) for _ in range(2)]
        for k in range(D // HEAD):
            wide = x_ref[rows, k * HEAD:(k + 1) * HEAD].astype(jnp.float32)
            squares[k % 2] = squares[k % 2] + wide * wide
        inv = lax.rsqrt(jnp.sum(squares[0] + squares[1], axis=-1, keepdims=True) * (1.0 / D) + NORM_EPS)
        for k in range(D // HEAD):
            cols = slice(k * HEAD, (k + 1) * HEAD)
            wide = x_ref[rows, cols].astype(jnp.float32)
            h_ref[rows, cols] = (wide * inv * gain_ref[cols].astype(jnp.float32).reshape(1, HEAD)).astype(jnp.bfloat16)
        return carry

    gain_copy.wait()
    for k in range(XCHUNKS):
        x_copies[k].wait()
        if k == 0:
            start_weights()
        lax.fori_loop(k * (ROWS // 16 // XCHUNKS), (k + 1) * (ROWS // 16 // XCHUNKS), norm_step, 0)
    pl.semaphore_wait(barrier, 1)

    def head_copy(head, n):
        return pltpu.make_async_remote_copy(src_ref=qkv.at[head], dst_ref=qkv.at[head], send_sem=s_q, recv_sem=r_q.at[n], device_id=partner, device_id_type=MESH)

    def proj_step(i, carry):
        pltpu.make_async_copy(wq_hbm.at[:, :TILE], wbuf.at[i], wsem.at[i]).wait()
        acc = jnp.dot(h_ref[...], wbuf[i], preferred_element_type=jnp.float32)
        for hh in range(2):
            part = acc[:, hh * HEAD:(hh + 1) * HEAD]
            turned = pltpu.roll(part, HEAD // 2, 1)
            cos_tab, sin_tab = turn[0], turn[1]
            if hh == 1:
                cos_tab = jnp.where(i > 0, cos_tab, 1.0)
                sin_tab = jnp.where(i > 0, sin_tab, 0.0)
            head = jnp.where(i == 0, HEADS + KV * hh + core, GROUP * core + 2 * (i - 1) + hh)
            qkv[head] = part * cos_tab + turned * sin_tab
            head_copy(head, 2 * i + hh).start()
        return carry

    lax.fori_loop(0, NTILE, proj_step, 0)
    for n in range(2 * NTILE):
        head_copy(0, n).wait_recv()
    half = qkv.at[pl.ds(0, 2 * NTILE)]
    pltpu.make_async_remote_copy(src_ref=half, dst_ref=half, send_sem=s_q, recv_sem=r_q.at[0], device_id=partner, device_id_type=MESH).wait_send()


def attend_kernel(ctx_ref, mask_ref, qkv, ck_hbm, cv_hbm,
                  o_ref, nk_hbm, nv_hbm,
                  kbuf, vbuf, ksem, vsem, nksem, nvsem):
    cp_rank = lax.axis_index('cp')

    def start_cache(r):
        pltpu.make_async_copy(ck_hbm.at[r, :, 0], kbuf.at[r], ksem.at[r]).start()
        pltpu.make_async_copy(cv_hbm.at[r, :, 0], vbuf.at[r], vsem.at[r]).start()

    def start_step(i):
        for k in range(UNROLL):
            start_cache(UNROLL * i + k)
        start_cache(EARLY + i)

    for i in range(STEPS_AHEAD):
        start_step(i)

    def prepare(r):
        pltpu.make_async_copy(ck_hbm.at[r, :, 0], kbuf.at[r], ksem.at[r]).wait()
        pltpu.make_async_copy(cv_hbm.at[r, :, 0], vbuf.at[r], vsem.at[r]).wait()
        ctx = ctx_ref[r]
        rows = pl.ds(pl.multiple_of(r * TREE, 8), TREE)
        first = ctx // BLK
        last = (ctx + TREE - 1) // BLK

        def insert(block):
            j = block // CP
            slot_of = lax.broadcasted_iota(jnp.int32, (BLK, TREE), 0) + (block * BLK - ctx)
            pick = (slot_of == lax.broadcasted_iota(jnp.int32, (BLK, TREE), 1)).astype(jnp.bfloat16)
            wide_slot = lax.broadcasted_iota(jnp.int32, (BLK, HEAD), 0) + (block * BLK - ctx)
            inside = (wide_slot >= 0) & (wide_slot < TREE)
            for hd in range(KV):
                for buf, base in ((kbuf, HEADS), (vbuf, HEADS + KV)):
                    new = qkv[base + hd, rows, :].astype(jnp.bfloat16)
                    placed = jnp.dot(pick, new, preferred_element_type=jnp.float32)
                    old = buf[r, j, hd].astype(jnp.float32)
                    buf[r, j, hd] = jnp.where(inside, placed, old).astype(jnp.bfloat16)

        @pl.when(lax.rem(first, CP) == cp_rank)
        def _():
            insert(first)

        @pl.when((lax.rem(last, CP) == cp_rank) & (last != first))
        def _():
            insert(last)

        pltpu.make_async_copy(kbuf.at[r], nk_hbm.at[r, :, 0], nksem.at[r]).start()
        pltpu.make_async_copy(vbuf.at[r], nv_hbm.at[r, :, 0], nvsem.at[r]).start()


    def raw_scores(r):
        ctx = ctx_ref[r]
        rows = pl.ds(pl.multiple_of(r * TREE, 8), TREE)
        lane = lax.broadcasted_iota(jnp.int32, (TREE, NBLK * BLK), 1)
        pos = (lane // BLK * CP + cp_rank) * BLK + lane % BLK - ctx
        onehot = (pos == lax.broadcasted_iota(jnp.int32, (TREE, NBLK * BLK), 0)).astype(jnp.bfloat16)
        allowed = jnp.dot(mask_ref[r].astype(jnp.float32).astype(jnp.bfloat16), onehot, preferred_element_type=jnp.float32)
        bias = jnp.where((pos < 0) | (allowed > 0.5), 0.0, MASKED)

        stats = jnp.zeros((TREE, HEAD), jnp.float32)
        stat_lane = lax.broadcasted_iota(jnp.int32, (TREE, HEAD), 1)
        scores = []
        for hd in range(KV):
            query = qkv[hd * GROUP:(hd + 1) * GROUP, rows, :].reshape(GROUP * TREE, HEAD).astype(jnp.bfloat16)
            keys = kbuf[r, :, hd].reshape(NBLK * BLK, HEAD)
            scores.append(lax.dot_general(query, keys, (((1,), (1,)), ((), ())), preferred_element_type=jnp.float32))
        return bias, stats, stat_lane, scores

    def finish(r, bias, stats, stat_lane, scores):
        for hd in range(KV):
            vals = vbuf[r, :, hd].reshape(NBLK * BLK, HEAD)
            score = scores[hd].reshape(GROUP, TREE, NBLK * BLK) * (HEAD ** -0.5 * LOG2E) + bias[None]
            top = jnp.max(score, axis=-1, keepdims=True)
            prob = jnp.exp2(score - top)
            total = jnp.sum(prob, axis=-1, keepdims=True)
            mixed = jnp.dot(prob.reshape(GROUP * TREE, NBLK * BLK).astype(jnp.bfloat16), vals, preferred_element_type=jnp.float32)
            for g in range(GROUP):
                head = hd * GROUP + g
                o_ref[r, :, head * HEAD:(head + 1) * HEAD] = mixed[g * TREE:(g + 1) * TREE]
                stats = jnp.where(stat_lane == head, top[g], stats)
                stats = jnp.where(stat_lane == HEADS + head, total[g], stats)
        o_ref[r, :, WIDE:] = stats


    def attend_step(i, carry):
        @pl.when(i + STEPS_AHEAD < EARLY // UNROLL)
        def _():
            start_step(i + STEPS_AHEAD)

        group = [i * UNROLL + k for k in range(UNROLL)]
        for r in group:
            prepare(r)
        held = [raw_scores(r) for r in group]
        for r, values in zip(group, held):
            finish(r, *values)
        prepare(EARLY + i)
        return carry

    lax.fori_loop(0, EARLY // UNROLL, attend_step, 0)

    def drain(r, carry):
        pltpu.make_async_copy(kbuf.at[r], nk_hbm.at[r, :, 0], nksem.at[r]).wait()
        pltpu.make_async_copy(vbuf.at[r], nv_hbm.at[r, :, 0], nvsem.at[r]).wait()
        return carry

    lax.fori_loop(0, REQ, drain, 0)


def merge(a, b):
    ta, tb = a[:, WIDE:], b[:, WIDE:]
    top = jnp.maximum(ta, tb)
    fa, fb = jnp.exp2(ta - top), jnp.exp2(tb - top)
    total = ta * pltpu.roll(fa, HEADS, 1) + tb * pltpu.roll(fb, HEADS, 1)
    lane = lax.broadcasted_iota(jnp.int32, (TREE, HEAD), 1)
    return fa, fb, total, jnp.where(lane < HEADS, top, total)


def main_kernel(ctx_ref, mask_ref, qkv, early, k_hbm, v_hbm, w_hbm, x_hbm, y_ref,
                kbuf, vbuf, late, pin, yrecv, heads, hbf, wbuf, xbuf,
                part, in_end, in_mid, fin, fin_y, fin_c, fin_cy,
                ksem, vsem, wsem, xsem, s_p, r_p, s_y, r_y, s_a, r_a,
                s_e, r_e, s_m, r_m, s_f, r_f, s_yf, r_yf, s_cf, r_cf, s_cy, r_cy):
    cp_rank = lax.axis_index('cp')
    z = lax.axis_index('tp')
    yy = cp_rank // 2
    core = cp_rank % 2
    other_core = 1 - core
    other_y = 1 - yy
    mid = (z + 1) // 2 % 2
    partner = {'cp': yy * 2 + other_core}
    across = {'cp': other_y * 2 + core}
    pair = {'tp': z + 1 - 2 * (z % 2)}
    middle = {'tp': 3 - z}

    def remote(src, dst, send, recv, peer):
        return pltpu.make_async_remote_copy(src_ref=src, dst_ref=dst, send_sem=send, recv_sem=recv, device_id=peer, device_id_type=MESH)

    barrier = pltpu.get_barrier_semaphore()
    for peer in (partner, across, pair):
        pl.semaphore_signal(barrier, inc=1, device_id=peer, device_id_type=MESH)

    @pl.when(mid == 1)
    def _():
        pl.semaphore_signal(barrier, inc=1, device_id=middle, device_id_type=MESH)

    for r in range(EARLY, REQ):
        slot = r - EARLY
        pltpu.make_async_copy(k_hbm.at[r, :, 0], kbuf.at[slot], ksem.at[slot]).start()
        pltpu.make_async_copy(v_hbm.at[r, :, 0], vbuf.at[slot], vsem.at[slot]).start()

    def weight_copy(j):
        cols = pl.ds(pl.multiple_of(core * HALF + j * W, W), W)
        return pltpu.make_async_copy(w_hbm.at[:, cols], wbuf.at[j], wsem.at[j])

    def start_weight(j, carry):
        weight_copy(j).start()
        return carry

    x_copies = [pltpu.make_async_copy(
        x_hbm.at[pl.ds(pl.multiple_of(w * WAVE_ROWS + yy * PART_ROWS, 16), PART_ROWS), pl.ds(pl.multiple_of(core * HALF, HALF), HALF)],
        xbuf.at[w], xsem.at[w]) for w in range(WAVES)]
    def raw_scores(r):
        slot = r - EARLY
        ctx = ctx_ref[r]
        rows = pl.ds(pl.multiple_of(r * TREE, 8), TREE)
        lane = lax.broadcasted_iota(jnp.int32, (TREE, NBLK * BLK), 1)
        pos = (lane // BLK * CP + cp_rank) * BLK + lane % BLK - ctx
        onehot = (pos == lax.broadcasted_iota(jnp.int32, (TREE, NBLK * BLK), 0)).astype(jnp.bfloat16)
        allowed = jnp.dot(mask_ref[r].astype(jnp.float32).astype(jnp.bfloat16), onehot, preferred_element_type=jnp.float32)
        bias = jnp.where((pos < 0) | (allowed > 0.5), 0.0, MASKED)
        scores = []
        for hd in range(KV):
            query = qkv[hd * GROUP:(hd + 1) * GROUP, rows, :].reshape(GROUP * TREE, HEAD).astype(jnp.bfloat16)
            keys = kbuf[slot, :, hd].reshape(NBLK * BLK, HEAD)
            scores.append(lax.dot_general(query, keys, (((1,), (1,)), ((), ())), preferred_element_type=jnp.float32))
        return bias, scores

    def attend(r, bias, scores):
        slot = r - EARLY
        stats = jnp.zeros((TREE, HEAD), jnp.float32)
        stat_lane = lax.broadcasted_iota(jnp.int32, (TREE, HEAD), 1)
        for hd in range(KV):
            vals = vbuf[slot, :, hd].reshape(NBLK * BLK, HEAD)
            score = scores[hd].reshape(GROUP, TREE, NBLK * BLK) * (HEAD ** -0.5 * LOG2E) + bias[None]
            top = jnp.max(score, axis=-1, keepdims=True)
            prob = jnp.exp2(score - top)
            total = jnp.sum(prob, axis=-1, keepdims=True)
            mixed = jnp.dot(prob.reshape(GROUP * TREE, NBLK * BLK).astype(jnp.bfloat16), vals, preferred_element_type=jnp.float32)
            for g in range(GROUP):
                head = hd * GROUP + g
                late[slot, :, head * HEAD:(head + 1) * HEAD] = mixed[g * TREE:(g + 1) * TREE]
                stats = jnp.where(stat_lane == head, top[g], stats)
                stats = jnp.where(stat_lane == HEADS + head, total[g], stats)
        late[slot, :, WIDE:] = stats

    def enter():
        @pl.when(mid == 1)
        def _():
            pl.semaphore_wait(barrier, 4)

        @pl.when(mid == 0)
        def _():
            pl.semaphore_wait(barrier, 3)

    def own(w, chip, to_core):
        return late.at[2 * chip + to_core] if w == WAVES - 1 else early.at[4 * w + 2 * chip + to_core]

    def chip_copy(w, side):
        chip = yy if side else other_y
        return remote(own(w, chip, other_core), pin.at[w, side], s_p.at[w, side], r_p.at[w, side], partner)

    def exchange(w):
        for side in (0, 1):
            chip_copy(w, side).start()

    def y_copy(w):
        return remote(pin.at[w, 0], yrecv.at[w], s_y.at[w], r_y.at[w], across)

    def blend(a, b):
        fa, fb, total, stats = merge(a, b)
        for h in range(HEADS):
            cols = slice(h * HEAD, (h + 1) * HEAD)
            b[:, cols] = a[:, cols] * fa[:, h:h + 1] + b[:, cols] * fb[:, h:h + 1]
        b[:, WIDE:] = stats

    def head_copy(w, owner):
        return remote(heads.at[w, owner], heads.at[w, owner], s_a.at[w], r_a.at[w], partner)

    def finish_start(w):
        y_copy(w).wait_recv()
        a, b, out = pin.at[w, 1], yrecv.at[w], heads.at[w, core]
        fa, fb, total, stats = merge(a, b)
        inv = 1.0 / total
        for h in range(HEADS):
            cols = slice(h * HEAD, (h + 1) * HEAD)
            mixed = a[:, cols] * fa[:, h:h + 1] + b[:, cols] * fb[:, h:h + 1]
            out[:, cols] = mixed * inv[:, HEADS + h:HEADS + h + 1]
        head_copy(w, core).start()

    def finish_end(w):
        head_copy(w, other_core).wait_recv()
        hbf[...] = heads[w].reshape(PART_ROWS, WIDE).astype(jnp.bfloat16)

    def blend_across(w):
        chip_copy(w, 0).wait_recv()
        blend(own(w, other_y, core), pin.at[w, 0])
        y_copy(w).start()

    def blend_mine(w):
        chip_copy(w, 1).wait_recv()
        blend(own(w, yy, core), pin.at[w, 1])

    def pair_step(i, carry):
        pair_of = [EARLY + UNROLL * i + k for k in range(UNROLL)]
        for r in pair_of:
            slot = r - EARLY
            pltpu.make_async_copy(k_hbm.at[r, :, 0], kbuf.at[slot], ksem.at[slot]).wait()
            pltpu.make_async_copy(v_hbm.at[r, :, 0], vbuf.at[slot], vsem.at[slot]).wait()

        @pl.when(i == 0)
        def _():
            lax.fori_loop(0, NP, start_weight, 0)
            for copy in x_copies:
                copy.start()

        held = [raw_scores(r) for r in pair_of]
        for r, values in zip(pair_of, held):
            attend(r, *values)

        @pl.when(i == 0)
        def _():
            blend_across(0)

        @pl.when(i == 1)
        def _():
            exchange(2)
            blend_across(1)
            blend_mine(0)
            blend_mine(1)
        return carry

    enter()
    exchange(0)
    exchange(1)
    lax.fori_loop(0, LATE // UNROLL, pair_step, 0)
    for copy in x_copies:
        copy.wait()
    finish_start(0)
    blend_across(2)
    finish_end(0)

    def end_copy(p):
        return remote(part.at[p], in_end.at[p], s_e, r_e.at[p], pair)

    def mid_copy(p):
        return remote(part.at[p], in_mid.at[p], s_m, r_m.at[p], middle)

    def fin_copy(p):
        return remote(fin.at[p], fin.at[p], s_f, r_f.at[p], pair)

    def across_copy(p):
        return remote(fin.at[p], fin_y.at[p], s_yf, r_yf.at[p], across)

    def core_copy(p):
        return remote(fin.at[p], fin_c.at[p], s_cf, r_cf.at[p], partner)

    def core_y_copy(p):
        return remote(fin_y.at[p], fin_cy.at[p], s_cy, r_cy.at[p], partner)

    def project(p):
        j = p % NP

        @pl.when(p < NP)
        def _():
            weight_copy(j).wait()

        prod = jnp.dot(hbf[...], wbuf[j], preferred_element_type=jnp.float32)
        part[p] = prod.astype(jnp.bfloat16).astype(jnp.float32)

        @pl.when(mid == 0)
        def _():
            end_copy(p).start()

    def emit(buf, p, chip, half):
        rows = pl.ds(pl.multiple_of(p // NP * WAVE_ROWS + chip * PART_ROWS, 16), PART_ROWS)
        cols = pl.ds(pl.multiple_of(half * HALF + p % NP * W, W), W)
        y_ref[rows, cols] = buf[p].astype(jnp.bfloat16)

    def take_end(p):
        end_copy(p).wait_recv()
        part[p] = part[p] + in_end[p]
        mid_copy(p).start()

    def take_mid(p):
        mid_copy(p).wait_recv()
        xcols = pl.ds(pl.multiple_of(p % NP * W, W), W)
        fin[p] = (part[p] + in_mid[p]) + xbuf[p // NP, :, xcols].astype(jnp.float32)
        fin_copy(p).start()
        across_copy(p).start()
        core_copy(p).start()
        emit(fin, p, yy, core)

    def take_fin(p):
        fin_copy(p).wait_recv()
        across_copy(p).start()
        core_copy(p).start()
        emit(fin, p, yy, core)

    def take_core(p):
        core_copy(p).wait_recv()
        emit(fin_c, p, yy, other_core)

    def take_across(p):
        across_copy(p).wait_recv()
        core_y_copy(p).start()
        emit(fin_y, p, other_y, core)

    def take_core_y(p):
        core_y_copy(p).wait_recv()
        emit(fin_cy, p, other_y, other_core)

    def ahead_step(p, carry):
        project(p)
        return carry

    lax.fori_loop(0, AHEAD, ahead_step, 0)
    blend_mine(2)
    lag = lambda at_mid, at_end: jnp.where(mid == 1, at_mid, at_end)
    lag_core, lag_across, lag_core_y = lag(6, 9), lag(8, 11), lag(10, 13)

    def step(s, carry):
        for w in range(1, WAVES):
            @pl.when(s == w * NP - AHEAD - 4)
            def _():
                finish_start(w)

            @pl.when(s == w * NP - AHEAD)
            def _():
                finish_end(w)

        @pl.when(s + AHEAD < PIECES)
        def _():
            project(s + AHEAD)

        @pl.when((mid == 1) & (s < PIECES))
        def _():
            take_end(s)

        @pl.when((mid == 1) & (s >= 3) & (s < PIECES + 3))
        def _():
            take_mid(s - 3)

        @pl.when((mid == 0) & (s >= 7) & (s < PIECES + 7))
        def _():
            take_fin(s - 7)

        for this_lag, body in ((lag_core, take_core), (lag_across, take_across), (lag_core_y, take_core_y)):
            p = s - this_lag

            @pl.when((p >= 0) & (p < PIECES))
            def _():
                body(p)
        return carry

    lax.fori_loop(0, PIECES + 13, step, 0)

    for w in range(WAVES):
        for side in (0, 1):
            chip_copy(w, side).wait_send()
        y_copy(w).wait_send()
        head_copy(w, core).wait_send()

    remote(fin, fin_y, s_yf, r_yf.at[0], across).wait_send()
    remote(fin, fin_c, s_cf, r_cf.at[0], partner).wait_send()
    remote(fin_y, fin_cy, s_cy, r_cy.at[0], partner).wait_send()

    @pl.when(mid == 1)
    def _():
        remote(part, in_mid, s_m, r_m.at[0], middle).wait_send()
        remote(fin, fin, s_f, r_f.at[0], pair).wait_send()

    @pl.when(mid == 0)
    def _():
        remote(part, in_end, s_e, r_e.at[0], pair).wait_send()


def solution(mesh):
    cache_spec = P('dp', None, 'cp', 'tp')
    row_spec = P('dp')
    anywhere = pl.BlockSpec(memory_space=pl.ANY)
    vmem = pl.BlockSpec(memory_space=pltpu.VMEM)
    smem = pl.BlockSpec(memory_space=pltpu.SMEM)
    dma = pltpu.SemaphoreType.DMA
    f32, bf16 = jnp.float32, jnp.bfloat16

    def local_step(hidden, attn_gain, w_query, w_key, w_value, w_out, cache_k, cache_v, ctx_len, positions, tree_mask):
        cos_tab, sin_tab = rope_tables(positions)
        flat = hidden.reshape(ROWS, D)
        cache_shape = jax.ShapeDtypeStruct(cache_k.shape, bf16)
        heads_qkv = pl.pallas_call(
            project_kernel,
            out_shape=pltpu.VMEM((HEADS + 2 * KV, ROWS, HEAD), f32),
            in_specs=[vmem, vmem, pl.BlockSpec(memory_space=pltpu.HBM)] + [anywhere] * 4,
            out_specs=vmem,
            scratch_shapes=[
                pltpu.VMEM((ROWS, D), bf16), pltpu.VMEM((D,), bf16), pltpu.VMEM((ROWS, D), bf16), pltpu.VMEM((2, ROWS, HEAD), f32), pltpu.VMEM((NTILE, D, TILE), bf16),
                dma((XCHUNKS,)), dma, dma((NTILE,)), dma, dma((2 * NTILE,)),
            ],
            compiler_params=pltpu.CompilerParams(vmem_limit_bytes=50 * 1024 * 1024, collective_id=1, has_side_effects=True),
            cost_estimate=pl.CostEstimate(flops=6_000_000_000, bytes_accessed=26_000_000, transcendentals=1_000),
            name='project',
        )(pltpu.with_memory_space_constraint(cos_tab, pltpu.VMEM), pltpu.with_memory_space_constraint(sin_tab, pltpu.VMEM), pltpu.with_memory_space_constraint(attn_gain, pltpu.HBM), flat, w_query, w_key, w_value)
        heads_qkv = pltpu.with_memory_space_constraint(heads_qkv, pltpu.VMEM)
        early_out, new_k, new_v = pl.pallas_call(
            attend_kernel,
            out_shape=(pltpu.VMEM((EARLY, TREE, EXT), f32), cache_shape, cache_shape),
            in_specs=[smem, vmem, vmem] + [anywhere] * 2,
            out_specs=(vmem, anywhere, anywhere),
            scratch_shapes=[
                pltpu.VMEM((REQ, NBLK, KV, BLK, HEAD), bf16), pltpu.VMEM((REQ, NBLK, KV, BLK, HEAD), bf16),
                dma((REQ,)), dma((REQ,)), dma((REQ,)), dma((REQ,)),
            ],
            compiler_params=pltpu.CompilerParams(vmem_limit_bytes=40 * 1024 * 1024),
            cost_estimate=pl.CostEstimate(flops=3_000_000_000, bytes_accessed=26_000_000, transcendentals=4_000_000),
            name='attend',
        )(ctx_len, tree_mask, heads_qkv, cache_k, cache_v)
        pieces = pltpu.VMEM((PIECES, PART_ROWS, W), f32)
        out = pl.pallas_call(
            main_kernel,
            out_shape=pltpu.VMEM((ROWS, D), bf16),
            in_specs=[smem, vmem, vmem, vmem] + [anywhere] * 4,
            out_specs=vmem,
            scratch_shapes=[
                pltpu.VMEM((LATE, NBLK, KV, BLK, HEAD), bf16), pltpu.VMEM((LATE, NBLK, KV, BLK, HEAD), bf16),
                pltpu.VMEM((LATE, TREE, EXT), f32), pltpu.VMEM((WAVES, 2, TREE, EXT), f32), pltpu.VMEM((WAVES, TREE, EXT), f32), pltpu.VMEM((WAVES, 2, TREE, WIDE), f32),
                pltpu.VMEM((PART_ROWS, WIDE), bf16), pltpu.VMEM((NP, WIDE, W), bf16), pltpu.VMEM((WAVES, PART_ROWS, HALF), bf16),
                pieces, pieces, pieces, pieces, pieces, pieces, pieces,
                dma((LATE,)), dma((LATE,)), dma((NP,)), dma((WAVES,)), dma((WAVES, 2)), dma((WAVES, 2)), dma((WAVES,)), dma((WAVES,)), dma((WAVES,)), dma((WAVES,)),
            ] + [dma, dma((PIECES,))] * 6,
            compiler_params=pltpu.CompilerParams(vmem_limit_bytes=50 * 1024 * 1024, collective_id=0, has_side_effects=True),
            cost_estimate=pl.CostEstimate(flops=5_000_000_000, bytes_accessed=42_000_000, transcendentals=5_000_000),
            name='main',
        )(ctx_len, tree_mask, heads_qkv, pltpu.with_memory_space_constraint(early_out, pltpu.VMEM), new_k, new_v, w_out, flat)
        return out.reshape(REQ, TREE, D), new_k, new_v

    return jax.shard_map(local_step, mesh=mesh, in_specs=(row_spec, P(), P(None, 'tp'), P(None, 'tp'), P(None, 'tp'), P('tp', None), cache_spec, cache_spec, row_spec, row_spec, row_spec), out_specs=(row_spec, cache_spec, cache_spec), check_vma=False)
```
